16 devices in a mesh: ey: 2 (over z), ex: 8 (over y, x, core).
Axes of the slice: x: 2, y: 2, z: 2, core: 2. Of those that a mesh axis runs over, the one named last changes fastest.
Arguments:
- x: bfloat16 [512, 2048], P(('ey', 'ex'))
- kv_k: bfloat16 [512, 256, 4, 128], P(('ey', 'ex'))
- kv_v: bfloat16 [512, 256, 4, 128], P(('ey', 'ex'))
- lens: int32 [512], P(('ey', 'ex'))
- topk_idx: int32 [512, 4], P(('ey', 'ex'))
- gates: float32 [512, 4], P(('ey', 'ex'))
- ln1: bfloat16 [2048], replicated
- wq: bfloat16 [2048, 4096], replicated
- wo: bfloat16 [4096, 2048], replicated
- ln2: bfloat16 [2048], replicated
- ws1: bfloat16 [2048, 5632], replicated
- ws3: bfloat16 [2048, 5632], replicated
- ws2: bfloat16 [5632, 2048], replicated
- w1: bfloat16 [64, 2048, 1408], P(('ey', 'ex'))
- w3: bfloat16 [64, 2048, 1408], P(('ey', 'ex'))
- w2: bfloat16 [64, 1408, 2048], P(('ey', 'ex'))
Outputs:
- output: bfloat16 [512, 2048], P(('ey', 'ex'))
All inputs are finite; a program needn't handle non-finite values.
Results may differ from the reference program's by a relative error of at most 0.0124499.
Values are sent between devices in bfloat16 or wider.
A program may use at most 1 GiB of HBM per device.

```python
import jax
import jax.numpy as jnp
from jax import lax

DEVICES = 16
B_DEV = 32
L = 256
D = 2048
HEADS = 32
KV_HEADS = 4
HEAD = 128
F = 1408
FS = 5632
E = 64
TOP = 4
EPS = 1e-6
B = DEVICES * B_DEV
E_DEV = E // DEVICES
CAP = B_DEV - B_DEV // 8
GROUP = HEADS // KV_HEADS


def _normal(key, shape, scale):
    return (scale * jax.random.normal(key, shape, jnp.float32)).astype(jnp.bfloat16)


def _route_ids(key):
    expert_ids = jnp.arange(E)
    cold_dev = (expert_ids >= 2 * E_DEV) & (expert_ids < 3 * E_DEV)
    weight = jnp.where(expert_ids >= E - 2, 1, jnp.where(cold_dev, E * 37 // 5, E)).astype(jnp.uint32)
    arrival = (jax.random.bits(key, (B, E), jnp.uint32) >> 12) * weight[None, :]
    return jnp.argsort(arrival, axis=-1)[:, :TOP].astype(jnp.int32)


def setup_inputs(seed: int = 0) -> dict:
    ks = jax.random.split(jax.random.PRNGKey(seed), 16)
    dk = jax.random.split(jax.random.fold_in(jax.random.PRNGKey(seed), 7), 3)
    dev = jnp.arange(B) // B_DEV
    far = (dev % 4) == 0
    far_len = jax.random.randint(dk[0], (B,), 3 * L // 4, L, jnp.int32)
    near_len = jax.random.randint(dk[1], (B,), 0, L // 16, jnp.int32)
    lens = jnp.clip(jnp.where(far, far_len, near_len), 1, L).astype(jnp.int32)
    topk_idx = _route_ids(dk[2])
    gates = 2.5 * jax.nn.softmax(0.5 * jax.random.normal(ks[5], (B, TOP), jnp.float32), axis=-1)
    return {
        "x": _normal(ks[0], (B, D), 1.0),
        "kv_k": _normal(ks[1], (B, L, KV_HEADS, HEAD), 2.0),
        "kv_v": _normal(ks[2], (B, L, KV_HEADS, HEAD), 1.0),
        "lens": lens,
        "topk_idx": topk_idx.astype(jnp.int32),
        "gates": gates,
        "ln1": (1.0 + 0.1 * jax.random.normal(ks[6], (D,), jnp.float32)).astype(jnp.bfloat16),
        "wq": _normal(ks[7], (D, HEADS * HEAD), D ** -0.5),
        "wo": _normal(ks[8], (HEADS * HEAD, D), (HEADS * HEAD) ** -0.5),
        "ln2": (1.0 + 0.1 * jax.random.normal(ks[9], (D,), jnp.float32)).astype(jnp.bfloat16),
        "ws1": _normal(ks[10], (D, FS), D ** -0.5),
        "ws3": _normal(ks[11], (D, FS), D ** -0.5),
        "ws2": _normal(ks[12], (FS, D), FS ** -0.5),
        "w1": _normal(ks[13], (E, D, F), D ** -0.5),
        "w3": _normal(ks[14], (E, D, F), D ** -0.5),
        "w2": _normal(ks[15], (E, F, D), F ** -0.5),
    }


def _rms(v, w):
    v32 = v.astype(jnp.float32)
    r = lax.rsqrt(jnp.mean(v32 * v32, axis=-1, keepdims=True) + EPS)
    return (v32 * r * w.astype(jnp.float32)).astype(jnp.bfloat16)


def _swiglu(a, w1, w3, w2):
    z1 = jnp.dot(a, w1, preferred_element_type=jnp.float32)
    z3 = jnp.dot(a, w3, preferred_element_type=jnp.float32)
    g = (jax.nn.silu(z1) * z3).astype(jnp.bfloat16)
    return jnp.dot(g, w2, preferred_element_type=jnp.float32)


def _attend(args):
    q, k, v, n = args
    s = jnp.einsum("kgh,lkh->kgl", q.astype(jnp.float32), k.astype(jnp.float32)) * HEAD ** -0.5
    s = jnp.where(jnp.arange(L) < n, s, -jnp.inf)
    p = jax.nn.softmax(s, axis=-1).astype(jnp.bfloat16)
    return jnp.einsum("kgl,lkh->kgh", p.astype(jnp.float32), v.astype(jnp.float32)).astype(jnp.bfloat16)


def reference(x, kv_k, kv_v, lens, topk_idx, gates, ln1, wq, wo, ln2, ws1, ws3, ws2, w1, w3, w2):
    a = _rms(x, ln1)
    q = jnp.dot(a, wq, preferred_element_type=jnp.float32).astype(jnp.bfloat16)
    o = lax.map(_attend, (q.reshape(B, KV_HEADS, GROUP, HEAD), kv_k, kv_v, lens))
    attn = jnp.dot(o.reshape(B, HEADS * HEAD), wo, preferred_element_type=jnp.float32)
    h = (x.astype(jnp.float32) + attn).astype(jnp.bfloat16)
    u = _rms(h, ln2)
    shared = _swiglu(u, ws1, ws3, ws2)
    blk = topk_idx.reshape(DEVICES, B_DEV * TOP)
    oh = jax.nn.one_hot(blk, E, dtype=jnp.int32)
    rank = jnp.sum((jnp.cumsum(oh, axis=1) - oh) * oh, axis=-1)
    src = jnp.arange(DEVICES)[:, None]
    slot = jnp.where(rank < CAP, (blk * DEVICES + src) * CAP + rank, E * DEVICES * CAP).reshape(-1)
    tok = jnp.arange(B * TOP) // TOP
    tok_buf = jnp.full((E * DEVICES * CAP,), B, jnp.int32).at[slot].set(tok, mode="drop")
    gate_buf = jnp.zeros((E * DEVICES * CAP,), jnp.float32).at[slot].set(gates.reshape(-1), mode="drop")

    def expert(acc, xs):
        t, g, e1, e3, e2 = xs
        rows = jnp.take(u, t, axis=0, mode="fill", fill_value=0)
        out = _swiglu(rows, e1, e3, e2).astype(jnp.bfloat16).astype(jnp.float32)
        return acc.at[t].add(g[:, None] * out, mode="drop"), None

    routed, _ = lax.scan(expert, jnp.zeros((B, D), jnp.float32),
                         (tok_buf.reshape(E, DEVICES * CAP), gate_buf.reshape(E, DEVICES * CAP), w1, w3, w2))
    return (h.astype(jnp.float32) + shared + routed).astype(jnp.bfloat16)
```

```python
import functools

import jax
import jax.numpy as jnp
from jax import lax
from jax.experimental import pallas as pl
from jax.experimental.pallas import tpu as pltpu
from jax.sharding import PartitionSpec as P

EPS = 1e-6
GRP = ("ey", "ex")
F32 = jnp.float32
BF16 = jnp.bfloat16
MESH = pl.DeviceIdType.MESH
VMEM = pl.BlockSpec(memory_space=pltpu.VMEM)
SMEM = pl.BlockSpec(memory_space=pltpu.SMEM)
HBM = pl.BlockSpec(memory_space=pltpu.HBM)
DMA = pltpu.SemaphoreType.DMA
TOP = 4
EDEV = 4


def _rms(v32, w_ref):
    r = lax.rsqrt(jnp.mean(v32 * v32, axis=-1, keepdims=True) + EPS)
    return (v32 * r * w_ref[...].astype(F32)).astype(BF16)


def _silu_mul(z1, z3):
    return (jax.nn.silu(z1) * z3).astype(BF16)


def _attn_kernel(x_ref, ln1_ref, ln2_ref, lens_ref, wq_hbm, k_hbm, v_hbm, wo_hbm, h_ref, u_ref,
                 wq_v, k_v, v_v, wo_v, qs, os, ob, q_sem, k_sem, v_sem, o_sem):
    nq, _, qn = wq_v.shape
    nk, kb = k_v.shape[0], k_v.shape[1]
    no, _, on = wo_v.shape
    b = x_ref.shape[0]
    nh = qs.shape[0] // b
    rows = k_v.shape[2]

    def q_copy(i):
        return pltpu.make_async_copy(wq_hbm.at[:, pl.ds(pl.multiple_of(i * qn, qn), qn)], wq_v.at[i], q_sem.at[i])

    def k_copy(i):
        return pltpu.make_async_copy(k_hbm.at[i], k_v.at[i], k_sem.at[i])

    def v_copy(i):
        return pltpu.make_async_copy(v_hbm.at[i], v_v.at[i], v_sem.at[i])

    def o_copy(i):
        return pltpu.make_async_copy(wo_hbm.at[:, pl.ds(pl.multiple_of(i * on, on), on)], wo_v.at[i], o_sem.at[i])

    for i in range(nq):
        q_copy(i).start()
    a = _rms(x_ref[...].astype(F32), ln1_ref)

    @pl.loop(0, nq)
    def _(i):
        k_copy(i).start()
        v_copy(i).start()
        q_copy(i).wait()
        q = jnp.dot(a, wq_v[i], preferred_element_type=F32).astype(BF16).astype(F32)
        for j in range(qn // 128):
            qs[pl.ds(i * (qn // 128) + j, b, stride=nh), :] = q[:, j * 128:(j + 1) * 128]

    kvh = 4
    row = lax.broadcasted_iota(jnp.int32, (nh, rows), 1)
    head = lax.broadcasted_iota(jnp.int32, (nh, rows), 0)
    pos = jnp.where(row % kvh == head // (nh // kvh), row // kvh, rows)

    @pl.loop(0, nk)
    def _(i):
        o_copy(i).start()
        k_copy(i).wait()
        v_copy(i).wait()
        for j in range(kb):
            s_idx = i * kb + j
            q = qs[pl.ds(pl.multiple_of(s_idx * nh, nh), nh), :].astype(BF16)
            s = lax.dot_general(q, k_v[i, j], (((1,), (1,)), ((), ())), preferred_element_type=F32) * 128 ** -0.5
            s = jnp.where(pos < lens_ref[s_idx], s, -jnp.inf)
            m = jnp.max(s, axis=-1, keepdims=True)
            p = jnp.exp(s - m)
            p = (p / jnp.sum(p, axis=-1, keepdims=True)).astype(BF16)
            os[pl.ds(pl.multiple_of(s_idx * nh, nh), nh), :] = jnp.dot(p, v_v[i, j], preferred_element_type=F32)

    for hh in range(nh):
        ob[:, hh * 128:(hh + 1) * 128] = os[pl.ds(hh, b, stride=nh), :].astype(BF16)

    for i in range(no):
        o_copy(i).wait()
        sl = slice(i * on, (i + 1) * on)
        attn = jnp.dot(ob[...], wo_v[i], preferred_element_type=F32)
        h_ref[:, sl] = (x_ref[:, sl].astype(F32) + attn).astype(BF16)
    u_ref[...] = _rms(h_ref[...].astype(F32), ln2_ref)


def _attention(x, k, v, lens, ln1, ln2, wq, wo):
    b, d = x.shape
    nqk = wq.shape[1]
    rows = k.shape[1] * k.shape[2]
    nq = nk = no = 8
    k = k.reshape(nk, b // nk, rows, 128)
    v = v.reshape(nk, b // nk, rows, 128)
    nh = nqk // 128
    return pl.pallas_call(
        _attn_kernel,
        out_shape=[jax.ShapeDtypeStruct((b, d), BF16)] * 2,
        in_specs=[VMEM, VMEM, VMEM, SMEM, HBM, HBM, HBM, HBM],
        out_specs=[VMEM, VMEM],
        scratch_shapes=[
            pltpu.VMEM((nq, d, nqk // nq), BF16),
            pltpu.VMEM((nk, b // nk, rows, 128), BF16),
            pltpu.VMEM((nk, b // nk, rows, 128), BF16),
            pltpu.VMEM((no, nqk, d // no), BF16),
            pltpu.VMEM((b * nh, 128), F32),
            pltpu.VMEM((b * nh, 128), F32),
            pltpu.VMEM((b, nqk), BF16),
            DMA((nq,)), DMA((nk,)), DMA((nk,)), DMA((no,)),
        ],
        compiler_params=pltpu.CompilerParams(vmem_limit_bytes=62 * 2 ** 20),
        name="attn",
    )(x, ln1.reshape(1, d), ln2.reshape(1, d), lens, wq, k, v, wo)


def _place():
    z = lax.axis_index("ey")
    ex = lax.axis_index("ex")
    return z, ex // 4, (ex // 2) % 2, ex % 2


def _dev(z, y, x, c):
    return (z, y * 4 + x * 2 + c)


def _flip(v, f):
    return 1 - v if f else v


def _offset(place, d):
    z, y, x = place
    return _flip(z, d // 4), _flip(y, (d // 2) % 2), _flip(x, d % 2)


def _gather_kernel(u_ref, m_ref, w1_hbm, w3_hbm, uall_hbm, mall_ref, g_ref,
                   ua, ma, w1_v, w3_v, w1_sem, w3_sem, out_sem,
                   us_send, us_recv, uf_send, uf_recv, ms_send, ms_recv, mf_send, mf_recv):
    z, y, x, c = _place()
    nw, _, wn = w1_v.shape

    def w_copy(hbm, vm, sem, i):
        return pltpu.make_async_copy(hbm.at[:, pl.ds(i * wn, wn)], vm.at[i], sem.at[i])

    for i in range(nw):
        w_copy(w1_hbm, w1_v, w1_sem, i).start()
        w_copy(w3_hbm, w3_v, w3_sem, i).start()
    barrier = pltpu.get_barrier_semaphore()
    for d in range(1, 8):
        oz, oy, ox = _offset((z, y, x), d)
        pl.semaphore_signal(barrier, inc=1, device_id=_dev(oz, oy, ox, c), device_id_type=MESH)
    pl.semaphore_signal(barrier, inc=1, device_id=_dev(z, y, x, 1 - c), device_id_type=MESH)
    pl.semaphore_wait(barrier, 8)

    me = ((z * 2 + y) * 2 + x) * 2 + c

    def sends(d):
        dev = _dev(*_offset((z, y, x), d), c) if d else _dev(z, y, x, 1 - c)
        return (pltpu.make_async_remote_copy(u_ref, ua.at[me], us_send.at[d], us_recv.at[d], device_id=dev,
                                             device_id_type=MESH),
                pltpu.make_async_remote_copy(m_ref, ma.at[me], ms_send.at[d], ms_recv.at[d], device_id=dev,
                                             device_id_type=MESH))

    def forwards(d):
        oz, oy, ox = _offset((z, y, x), d)
        src = ((oz * 2 + oy) * 2 + ox) * 2 + c
        dev = _dev(z, y, x, 1 - c)
        return (pltpu.make_async_remote_copy(ua.at[src], ua.at[src], uf_send.at[d], uf_recv.at[d], device_id=dev,
                                             device_id_type=MESH),
                pltpu.make_async_remote_copy(ma.at[src], ma.at[src], mf_send.at[d], mf_recv.at[d], device_id=dev,
                                             device_id_type=MESH))

    order = (7, 6, 5, 3, 4, 2, 1, 0)
    for d in order:
        for cp in sends(d):
            cp.start()
    ua[me] = u_ref[...]
    ma[me] = m_ref[...]

    fwd = list(order[:-1])
    for i in range(nw):
        w_copy(w1_hbm, w1_v, w1_sem, i).wait()
        w_copy(w3_hbm, w3_v, w3_sem, i).wait()
        z1 = jnp.dot(u_ref[...], w1_v[i], preferred_element_type=F32)
        z3 = jnp.dot(u_ref[...], w3_v[i], preferred_element_type=F32)
        g_ref[:, i * wn:(i + 1) * wn] = _silu_mul(z1, z3)
        if i >= nw - 7:
            d = fwd.pop(0)
            for s, f in zip(sends(d), forwards(d)):
                s.wait_recv()
                f.start()
    for d in fwd:
        for s, f in zip(sends(d), forwards(d)):
            s.wait_recv()
            f.start()
    for cp in sends(0):
        cp.wait_recv()
    for d in range(1, 8):
        for f in forwards(d):
            f.wait_recv()
    for d in range(8):
        for s in sends(d):
            s.wait_send()
        if d:
            for f in forwards(d):
                f.wait_send()
    out = pltpu.make_async_copy(ua, uall_hbm, out_sem)
    out.start()
    mall_ref[...] = ma[...]
    out.wait()


def _gather(u, meta, ws1, ws3):
    b, d = u.shape
    fs = ws1.shape[1]
    nw = 11
    return pl.pallas_call(
        _gather_kernel,
        out_shape=[jax.ShapeDtypeStruct((16, b, d), BF16), jax.ShapeDtypeStruct((16, b, 128), F32),
                   jax.ShapeDtypeStruct((b, fs), BF16)],
        in_specs=[VMEM, VMEM, HBM, HBM],
        out_specs=[HBM, VMEM, VMEM],
        scratch_shapes=[
            pltpu.VMEM((16, b, d), BF16),
            pltpu.VMEM((16, b, 128), F32),
            pltpu.VMEM((nw, d, fs // nw), BF16),
            pltpu.VMEM((nw, d, fs // nw), BF16),
            DMA((nw,)), DMA((nw,)), DMA(()),
            DMA((8,)), DMA((8,)), DMA((8,)), DMA((8,)), DMA((8,)), DMA((8,)), DMA((8,)), DMA((8,)),
        ],
        compiler_params=pltpu.CompilerParams(vmem_limit_bytes=62 * 2 ** 20, collective_id=0, has_side_effects=True),
        name="dispatch",
    )(u, meta, ws1, ws3)


SMALL = 32
GROUP = 256


def _expert_kernel(cap, blk, u_ref, m_ref, w1_hbm, w3_hbm, w2_hbm, p_ref,
                   w1_v, w3_v, w2_v, kcol, gcol, krow, cnt, order, w_sem):
    t, d = u_ref.shape
    ng = t // GROUP
    big = cap * (GROUP // blk)
    base = (lax.axis_index("ey") * 8 + lax.axis_index("ex")) * EDEV

    lane = lax.broadcasted_iota(jnp.int32, (t, 128), 1).astype(F32) + base.astype(F32)
    hit = jnp.zeros((t, 128), F32)
    gate = jnp.zeros((t, 128), F32)
    for j in range(TOP):
        same = m_ref[:, j:j + 1] == lane
        hit += jnp.where(same, 1.0, 0.0)
        gate += jnp.where(same, m_ref[:, TOP + j:TOP + j + 1], 0.0)
    r0 = lax.broadcasted_iota(jnp.int32, (GROUP, GROUP), 0)
    r1 = lax.broadcasted_iota(jnp.int32, (GROUP, GROUP), 1)
    before = jnp.where(r1 < r0, 1.0, 0.0)
    before_blk = jnp.where(r1 // blk == r0 // blk, before, 0.0).astype(BF16)
    before = before.astype(BF16)
    for g in range(ng):
        sl = slice(g * GROUP, (g + 1) * GROUP)
        rank = jnp.dot(before_blk, hit[sl].astype(BF16), preferred_element_type=F32)
        keep = jnp.where(rank < cap, hit[sl], 0.0)
        pos = jnp.dot(before, keep.astype(BF16), preferred_element_type=F32)
        key = jnp.where(keep > 0.0, pos, -1.0)
        krow[:, sl] = key.T[0:8]
        tot = jnp.sum(keep, axis=0, keepdims=True)
        for e in range(EDEV):
            kcol[e, sl] = jnp.broadcast_to(key[:, e:e + 1], (GROUP, 128))
            gcol[e, sl] = jnp.broadcast_to(gate[sl, e:e + 1], (GROUP, 128))
            cnt[e * ng + g] = jnp.sum(tot[:, e:e + 1]).astype(jnp.int32)
    for e in range(EDEV):
        n = cnt[e * ng] + cnt[e * ng + 1]
        rank = 0
        for f in range(EDEV):
            if f != e:
                m = cnt[f * ng] + cnt[f * ng + 1]
                rank += ((m >= n) if f < e else (m > n)).astype(jnp.int32)
        order[rank] = e

    def copies(i):
        e, s = order[i], lax.rem(i, 2)
        return (pltpu.make_async_copy(w1_hbm.at[e], w1_v.at[s], w_sem.at[s, 0]),
                pltpu.make_async_copy(w3_hbm.at[e], w3_v.at[s], w_sem.at[s, 1]),
                pltpu.make_async_copy(w2_hbm.at[e], w2_v.at[s], w_sem.at[s, 2]))

    for i in range(2):
        for cp in copies(i):
            cp.start()
    p_ref[...] = jnp.zeros_like(p_ref)

    def swiglu(rows, s):
        z1 = jnp.dot(rows, w1_v[s], preferred_element_type=F32)
        z3 = jnp.dot(rows, w3_v[s], preferred_element_type=F32)
        return jnp.dot(_silu_mul(z1, z3), w2_v[s], preferred_element_type=F32).astype(BF16)

    def pick(e, g, n):
        r = lax.broadcasted_iota(jnp.int32, (n, GROUP), 0).astype(F32)
        sel = jnp.where(krow[pl.ds(e, 1), pl.ds(pl.multiple_of(g * GROUP, GROUP), GROUP)] == r, 1.0, 0.0).astype(BF16)
        rows = u_ref[pl.ds(pl.multiple_of(g * GROUP, GROUP), GROUP), :]
        return jnp.dot(sel, rows, preferred_element_type=F32).astype(BF16)

    def put(e, g, n, out):
        tl = pl.ds(pl.multiple_of(g * GROUP, GROUP), GROUP)
        r = lax.broadcasted_iota(jnp.int32, (GROUP, 128), 1).astype(F32)
        key = kcol[e, tl]
        sel = jnp.concatenate([jnp.where(key == r + 128.0 * q, 1.0, 0.0) for q in range(-(-n // 128))], axis=1)
        sel = sel[:, :n].astype(BF16)
        gt = gcol[e, tl]
        for q in range(d // 256):
            cs = slice(q * 256, (q + 1) * 256)
            back = jnp.dot(sel, out[:, cs], preferred_element_type=F32)
            p_ref[tl, cs] += back * jnp.concatenate([gt, gt], axis=1)

    @pl.loop(0, EDEV)
    def _(i):
        e, s = order[i], lax.rem(i, 2)
        for cp in copies(i):
            cp.wait()
        most = jnp.maximum(cnt[e * ng], cnt[e * ng + 1])

        @pl.when(jnp.logical_and(most > 0, most <= SMALL))
        def _():
            rows = jnp.concatenate([pick(e, g, SMALL) for g in range(ng)], axis=0)
            out = swiglu(rows, s)
            for g in range(ng):
                put(e, g, SMALL, out[g * SMALL:(g + 1) * SMALL])

        @pl.when(most > SMALL)
        def _():
            @pl.loop(0, ng)
            def _(g):
                put(e, g, big, swiglu(pick(e, g, big), s))

        @pl.when(i + 2 < EDEV)
        def _():
            for cp in copies(i + 2):
                cp.start()


def _experts(u, meta, w1, w3, w2, blk):
    t, d = u.shape
    f = w1.shape[2]
    cap = blk - blk // 8
    ng = t // GROUP
    return pl.pallas_call(
        functools.partial(_expert_kernel, cap, blk),
        out_shape=jax.ShapeDtypeStruct((t, d), F32),
        in_specs=[VMEM, VMEM, HBM, HBM, HBM],
        out_specs=VMEM,
        scratch_shapes=[
            pltpu.VMEM((2, d, f), BF16),
            pltpu.VMEM((2, d, f), BF16),
            pltpu.VMEM((2, f, d), BF16),
            pltpu.VMEM((EDEV, t, 128), F32),
            pltpu.VMEM((EDEV, t, 128), F32),
            pltpu.VMEM((8, t), F32),
            pltpu.SMEM((EDEV * ng,), jnp.int32),
            pltpu.SMEM((EDEV,), jnp.int32),
            DMA((2, 3)),
        ],
        compiler_params=pltpu.CompilerParams(vmem_limit_bytes=62 * 2 ** 20),
        name="experts",
    )(u, meta, w1, w3, w2)


COLS = ((0, 640), (640, 640), (1280, 768))


def _combine_kernel(p_hbm, g_ref, h_ref, w_hbm, y_ref,
                    acc, r0, r1, r2, r3, w_v, sh, w_sem, p_sem,
                    s0, q0, s1, q1, s2, q2, s3, q3):
    z, y, x, c = _place()
    nw, _, wn = w_v.shape

    def w_copy(i):
        return pltpu.make_async_copy(w_hbm.at[:, pl.ds(i * wn, wn)], w_v.at[i], w_sem.at[i])

    streams = [(p, half) for half in range(2) for p in range(3)]
    place = {0: x, 1: y, 2: z}

    def cols(p):
        return pl.ds(COLS[p][0], COLS[p][1])

    def rows(half):
        return pl.ds(half * 16, 16)

    def load(k):
        p, half = streams[k]
        return pltpu.make_async_copy(p_hbm.at[:, :, :, c, rows(half), cols(p)], acc.at[:, :, :, rows(half), cols(p)],
                                     p_sem.at[k])

    def swap(k):
        p, half = streams[k]
        return pltpu.make_async_remote_copy(
            p_hbm.at[:, :, :, 1 - c, rows(half), cols(p)], r0.at[:, :, :, rows(half), cols(p)], s0.at[k], q0.at[k],
            device_id=_dev(z, y, x, 1 - c), device_id_type=MESH)

    def region(ref, p, half, step, mine):
        ix = [pl.ds(0, 2)] * 3
        for s in range(step):
            dim = (p + s) % 3
            v = place[dim]
            ix[2 - dim] = v if (s < step - 1 or mine) else 1 - v
        return ref.at[ix[0], ix[1], ix[2], rows(half), cols(p)]

    def landing(p, half, step):
        ref = (r1, r2, r3)[step - 1]
        if step == 1:
            return ref.at[:, :, rows(half), cols(p)]
        if step == 2:
            return ref.at[:, rows(half), cols(p)]
        return ref.at[rows(half), cols(p)]

    def hop(k, step):
        p, half = streams[k]
        dim = (p + step - 1) % 3
        o = [z, y, x]
        o[2 - dim] = 1 - o[2 - dim]
        send, recv = ((s1, q1), (s2, q2), (s3, q3))[step - 1]
        return pltpu.make_async_remote_copy(
            region(acc, p, half, step, False), landing(p, half, step), send.at[k], recv.at[k],
            device_id=_dev(*o, c), device_id_type=MESH)

    for k in range(6):
        load(k).start()
    barrier = pltpu.get_barrier_semaphore()
    pl.semaphore_signal(barrier, inc=1, device_id=_dev(z, y, x, 1 - c), device_id_type=MESH)
    for d in (1, 2, 4):
        pl.semaphore_signal(barrier, inc=1, device_id=_dev(*_offset((z, y, x), d), c), device_id_type=MESH)
    pl.semaphore_wait(barrier, 4)
    for k in range(6):
        swap(k).start()
    for i in range(nw):
        w_copy(i).start()

    def shared(i):
        w_copy(i).wait()
        cs = slice(i * wn, (i + 1) * wn)
        sh[:, cs] = jnp.dot(g_ref[...], w_v[i], preferred_element_type=F32) + h_ref[:, cs].astype(F32)

    for k in range(6):
        p, half = streams[k]
        load(k).wait()
        swap(k).wait_recv()
        rs, cs = slice(half * 16, half * 16 + 16), slice(COLS[p][0], COLS[p][0] + COLS[p][1])
        acc[:, :, :, rs, cs] += r0[:, :, :, rs, cs]
        hop(k, 1).start()
    shared(0)
    for k in range(6):
        p, half = streams[k]
        hop(k, 1).wait_recv()
        v = region(acc, p, half, 1, True)
        v[...] += landing(p, half, 1)[...]
        hop(k, 2).start()
    shared(1)
    shared(2)
    for k in range(6):
        p, half = streams[k]
        hop(k, 2).wait_recv()
        v = region(acc, p, half, 2, True)
        v[...] += landing(p, half, 2)[...]
        hop(k, 3).start()
    for i in range(3, nw):
        shared(i)
    for k in range(6):
        p, half = streams[k]
        hop(k, 3).wait_recv()
        v = region(acc, p, half, 3, True)
        tot = v[...] + landing(p, half, 3)[...]
        rs, cs = slice(half * 16, half * 16 + 16), slice(COLS[p][0], COLS[p][0] + COLS[p][1])
        y_ref[rs, cs] = (sh[rs, cs] + tot).astype(BF16)
    for k in range(6):
        swap(k).wait_send()
        for step in (1, 2, 3):
            hop(k, step).wait_send()


def _combine(part, g, h, ws2):
    b, d = h.shape
    fs = ws2.shape[0]
    nw = 8
    part = part.reshape(2, 2, 2, 2, b, d)
    return pl.pallas_call(
        _combine_kernel,
        out_shape=jax.ShapeDtypeStruct((b, d), BF16),
        in_specs=[HBM, VMEM, VMEM, HBM],
        out_specs=VMEM,
        scratch_shapes=[
            pltpu.VMEM((2, 2, 2, b, d), F32),
            pltpu.VMEM((2, 2, 2, b, d), F32),
            pltpu.VMEM((2, 2, b, d), F32),
            pltpu.VMEM((2, b, d), F32),
            pltpu.VMEM((b, d), F32),
            pltpu.VMEM((nw, fs, d // nw), BF16),
            pltpu.VMEM((b, d), F32),
            DMA((nw,)), DMA((6,)),
            DMA((6,)), DMA((6,)), DMA((6,)), DMA((6,)), DMA((6,)), DMA((6,)), DMA((6,)), DMA((6,)),
        ],
        compiler_params=pltpu.CompilerParams(vmem_limit_bytes=62 * 2 ** 20, collective_id=1, has_side_effects=True),
        name="combine",
    )(part, g, h, ws2)


def solution(mesh):
    def body(x, kv_k, kv_v, lens, idx, gates, ln1, wq, wo, ln2, ws1, ws3, ws2, w1, w3, w2):
        b, d = x.shape
        meta = jnp.concatenate([idx.astype(F32), gates, jnp.zeros((b, 128 - 2 * TOP), F32)], axis=1)
        h, u = _attention(x, kv_k, kv_v, lens, ln1, ln2, wq, wo)
        uall, mall, g = _gather(u, meta, ws1, ws3)
        part = _experts(uall.reshape(16 * b, d), mall.reshape(16 * b, 128), w1, w3, w2, b)
        return _combine(part, g, h, ws2)

    rows = P(GRP)
    rep = P()
    return jax.shard_map(
        body, mesh=mesh,
        in_specs=(rows, rows, rows, rows, rows, rows, rep, rep, rep, rep, rep, rep, rep, rows, rows, rows),
        out_specs=rows, check_vma=False)
```

```python
import functools

import jax
import jax.numpy as jnp
from jax import lax
from jax.experimental import pallas as pl
from jax.experimental.pallas import tpu as pltpu
from jax.sharding import PartitionSpec as P

EPS = 1e-6
GRP = ("ey", "ex")
F32 = jnp.float32
BF16 = jnp.bfloat16
MESH = pl.DeviceIdType.MESH
VMEM = pl.BlockSpec(memory_space=pltpu.VMEM)
SMEM = pl.BlockSpec(memory_space=pltpu.SMEM)
HBM = pl.BlockSpec(memory_space=pltpu.HBM)
DMA = pltpu.SemaphoreType.DMA
TOP = 4
EDEV = 4


def _rms(v32, w):
    r = lax.rsqrt(jnp.mean(v32 * v32, axis=-1, keepdims=True) + EPS)
    return (v32 * r * w.astype(F32)).astype(BF16)


def _silu_mul(z1, z3):
    return (jax.nn.silu(z1) * z3).astype(BF16)


def _place():
    z = lax.axis_index("ey")
    ex = lax.axis_index("ex")
    return z, ex // 4, (ex // 2) % 2, ex % 2


def _dev(z, y, x, c):
    return (z, y * 4 + x * 2 + c)


def _flip(v, f):
    return 1 - v if f else v


def _offset(place, d):
    z, y, x = place
    return _flip(z, d // 4), _flip(y, (d // 2) % 2), _flip(x, d % 2)


CH = 512
RING = 18
GROUP = 256


def _front_kernel(cap, x_ref, ln1_ref, ln2_ref, idx_ref, gate_ref, lens_ref, wq_hbm, k_hbm, v_hbm, wo_hbm, ws1_hbm,
                  ws3_hbm, h_ref, uall_hbm, g_ref, key_ref, gsel_ref, krow_ref, cnt_ref,
                  ring, k_v, v_v, qs, sc, ob, us, ua, ms, ma, hit,
                  r_sem, k_sem, v_sem, out_sem, us_send, us_recv, uf_send, uf_recv, ms_send, ms_recv):
    b, d = x_ref.shape
    nqk = wq_hbm.shape[1]
    nh = nqk // 128
    nq = nqk // CH
    nk, kb, rows = k_v.shape[:3]
    nw = ws1_hbm.shape[1] // CH
    z, y, x, c = _place()
    me = ((z * 2 + y) * 2 + x) * 2 + c

    def cols(i):
        return pl.ds(i * CH if isinstance(i, int) else pl.multiple_of(i * CH, CH), CH)

    def chunk(src, n):
        s = lax.rem(n, RING)
        return pltpu.make_async_copy(src, ring.at[s], r_sem.at[s])

    def q_copy(i):
        return chunk(wq_hbm.at[:, cols(i)], i)

    def o_copy(i):
        return chunk(wo_hbm.at[pl.ds(pl.multiple_of((i % 2) * d, d), d), cols(i // 2)], nq + i)

    def w_copies(i):
        return chunk(ws1_hbm.at[:, cols(i)], 2 * nq + 2 * i), chunk(ws3_hbm.at[:, cols(i)], 2 * nq + 2 * i + 1)

    def k_copy(i):
        return pltpu.make_async_copy(k_hbm.at[i], k_v.at[i], k_sem.at[i])

    def v_copy(i):
        return pltpu.make_async_copy(v_hbm.at[i], v_v.at[i], v_sem.at[i])

    for i in range(nq):
        q_copy(i).start()
    barrier = pltpu.get_barrier_semaphore()
    peers = [_dev(*_offset((z, y, x), o % 8), _flip(c, o // 8)) for o in range(1, 16)]
    for dev in peers:
        pl.semaphore_signal(barrier, inc=1, device_id=dev, device_id_type=MESH)
    ms[...] = jnp.zeros_like(ms)
    ms[0:TOP, 0:b] = idx_ref[...].astype(F32)
    ms[TOP:2 * TOP, 0:b] = gate_ref[...]
    a = _rms(x_ref[...].astype(F32), _row(ln1_ref))

    @pl.loop(0, nq)
    def _(i):
        k_copy(i).start()
        v_copy(i).start()
        o_copy(i).start()
        q_copy(i).wait()
        q = jnp.dot(a, ring[i], preferred_element_type=F32).astype(BF16).astype(F32)
        for j in range(CH // 128):
            qs[pl.ds(i * (CH // 128) + j, b, stride=nh), :] = q[:, j * 128:(j + 1) * 128]

    pl.semaphore_wait(barrier, 15)

    def m_send(o):
        return pltpu.make_async_remote_copy(ms, ma.at[me], ms_send.at[o], ms_recv.at[o], device_id=peers[o - 1],
                                            device_id_type=MESH)

    for o in range(1, 16):
        m_send(o).start()
    ma[me] = ms[...]

    kvh = 4
    row = lax.broadcasted_iota(jnp.int32, (nh, rows), 1)
    head = lax.broadcasted_iota(jnp.int32, (nh, rows), 0)
    pos = jnp.where(row % kvh == head // (nh // kvh), row // kvh, rows)

    def of(i):
        return pl.ds(pl.multiple_of(i * nh, nh), nh)

    @pl.loop(0, nk // 2)
    def _(i):
        for cp in w_copies(i):
            cp.start()
        for t in range(2):
            k_copy(i * 2 + t).wait()
            v_copy(i * 2 + t).wait()
        seqs = [(i * 2 + t, j, (i * 2 + t) * kb + j) for t in range(2) for j in range(kb)]
        for n, (ch, j, b_i) in enumerate(seqs):
            q = qs[of(b_i), :].astype(BF16)
            s = lax.dot_general(q, k_v[ch, j], (((1,), (1,)), ((), ())), preferred_element_type=F32) * 128 ** -0.5
            sc[n] = jnp.where(pos < lens_ref[b_i], s, -jnp.inf)
        ps = []
        for n in range(len(seqs)):
            s = sc[n]
            p = jnp.exp(s - jnp.max(s, axis=-1, keepdims=True))
            ps.append((p * (1.0 / jnp.sum(p, axis=-1, keepdims=True))).astype(BF16))
        for p, (ch, j, b_i) in zip(ps, seqs):
            qs[of(b_i), :] = jnp.dot(p, v_v[ch, j], preferred_element_type=F32)

    ahead = nk // 2
    while 2 * (ahead + 1) + nq <= RING:
        for cp in w_copies(ahead):
            cp.start()
        ahead += 1

    for hh in range(nh):
        ob[:, hh * 128:(hh + 1) * 128] = qs[pl.ds(hh, b, stride=nh), :].astype(BF16)

    no = d // CH

    @pl.loop(0, no)
    def _(i):
        acc = x_ref[:, cols(i)].astype(F32)
        attn = jnp.zeros((b, CH), F32)
        for t in range(2):
            o_copy(i * 2 + t).wait()
            attn += jnp.dot(ob[:, t * d:(t + 1) * d], ring[lax.rem(nq + i * 2 + t, RING)], preferred_element_type=F32)
        h_ref[:, cols(i)] = (acc + attn).astype(BF16)
        for cp in w_copies(ahead + i):
            cp.start()

    ahead += no
    us[...] = _rms(h_ref[...].astype(F32), _row(ln2_ref))

    def shared(i):
        c1, c3 = w_copies(i)
        c1.wait()
        c3.wait()
        s = lax.rem(2 * nq + 2 * i, RING)
        z1 = jnp.dot(us[...], ring[s], preferred_element_type=F32)
        z3 = jnp.dot(us[...], ring[s + 1], preferred_element_type=F32)
        g_ref[:, cols(i)] = _silu_mul(z1, z3)

    shared(0)

    def send(o):
        dev = _dev(*_offset((z, y, x), o), c) if o else _dev(z, y, x, 1 - c)
        return pltpu.make_async_remote_copy(us, ua.at[me], us_send.at[o], us_recv.at[o], device_id=dev,
                                            device_id_type=MESH)

    def source(o, core):
        oz, oy, ox = _offset((z, y, x), o)
        return ((oz * 2 + oy) * 2 + ox) * 2 + core

    def forward(o):
        src = source(o, c)
        return pltpu.make_async_remote_copy(ua.at[src], ua.at[src], uf_send.at[o], uf_recv.at[o],
                                            device_id=_dev(z, y, x, 1 - c), device_id_type=MESH)

    def store(o, core):
        src = source(o, core)
        return pltpu.make_async_copy(ua.at[src], uall_hbm.at[src], out_sem.at[2 * o + (0 if core is c else 1)])

    order = (7, 6, 5, 3, 4, 2, 1, 0)
    for o in order:
        send(o).start()
    ua[me] = us[...]
    n = 0
    while ahead < nw:
        for cp in w_copies(ahead):
            cp.start()
        ahead += 1
        n += 1
        if ahead < nw:
            shared(n)

    for o in range(1, 16):
        m_send(o).wait_recv()
    base = ((lax.axis_index("ey") * 8 + lax.axis_index("ex")) * EDEV).astype(F32)
    turned = ma[...].reshape(128, 128).T
    lane = lax.broadcasted_iota(jnp.int32, (b, 128), 1).astype(F32) + base
    nblk = ma.shape[0]
    for i in range(nblk):
        hb = jnp.zeros((b, 128), F32)
        gb = jnp.zeros((b, 128), F32)
        for j in range(TOP):
            at = i * 2 * TOP + j
            same = turned[0:b, at:at + 1] == lane
            hb += jnp.where(same, 1.0, 0.0)
            gb += jnp.where(same, turned[0:b, at + TOP:at + TOP + 1], 0.0)
        hit[i * b:(i + 1) * b, :] = hb
        gsel_ref[i * b:(i + 1) * b, :] = gb
    r0 = lax.broadcasted_iota(jnp.int32, (GROUP, GROUP), 0)
    r1 = lax.broadcasted_iota(jnp.int32, (GROUP, GROUP), 1)
    before = jnp.where(r1 < r0, 1.0, 0.0)
    before_blk = jnp.where(r1 // b == r0 // b, before, 0.0).astype(BF16)
    before = before.astype(BF16)
    for g in range(nblk * b // GROUP):
        sl = slice(g * GROUP, (g + 1) * GROUP)
        rank = jnp.dot(before_blk, hit[sl, :].astype(BF16), preferred_element_type=F32)
        keep = jnp.where(rank < cap, hit[sl, :], 0.0)
        at = jnp.dot(before, keep.astype(BF16), preferred_element_type=F32)
        key = jnp.where(keep > 0.0, at, -1.0)
        key_ref[sl, :] = key
        krow_ref[:, sl] = key.T[0:8]
        cnt_ref[g:g + 1, :] = jnp.sum(keep, axis=0, keepdims=True).astype(jnp.int32)

    fwd = list(order[:-1])
    for i in range(n if n else 1, nw):
        shared(i)
        if i >= nw - 6:
            o = fwd.pop(0)
            send(o).wait_recv()
            forward(o).start()
            store(o, c).start()
    for o in fwd:
        send(o).wait_recv()
        forward(o).start()
        store(o, c).start()
    store(0, c).start()
    send(0).wait_recv()
    store(0, 1 - c).start()
    for o in order[:-1]:
        forward(o).wait_recv()
        store(o, 1 - c).start()
    for o in range(8):
        send(o).wait_send()
        store(o, c).wait()
        store(o, 1 - c).wait()
        if o:
            forward(o).wait_send()
    for o in range(1, 16):
        m_send(o).wait_send()


def _row(ref):
    return jnp.concatenate([ref[i:i + 1, :] for i in range(ref.shape[0])], axis=1)


def _front(x, k, v, lens, idx, gates, ln1, ln2, wq, wo, ws1, ws3):
    b, d = x.shape
    nqk, fs = wq.shape[1], ws1.shape[1]
    rows = k.shape[1] * k.shape[2]
    nk = 8
    ndev = 16
    k = k.reshape(nk, b // nk, rows, 128)
    v = v.reshape(nk, b // nk, rows, 128)
    nh = nqk // 128
    t = ndev * b
    return pl.pallas_call(
        functools.partial(_front_kernel, b - b // 8),
        out_shape=[jax.ShapeDtypeStruct((b, d), BF16), jax.ShapeDtypeStruct((ndev, b, d), BF16),
                   jax.ShapeDtypeStruct((b, fs), BF16), jax.ShapeDtypeStruct((t, 128), F32),
                   jax.ShapeDtypeStruct((t, 128), F32), jax.ShapeDtypeStruct((8, t), F32),
                   jax.ShapeDtypeStruct((t // GROUP, 128), jnp.int32)],
        in_specs=[VMEM] * 5 + [SMEM] + [HBM] * 6,
        out_specs=[VMEM, HBM] + [VMEM] * 5,
        scratch_shapes=[
            pltpu.VMEM((RING, d, CH), BF16),
            pltpu.VMEM((nk, b // nk, rows, 128), BF16),
            pltpu.VMEM((nk, b // nk, rows, 128), BF16),
            pltpu.VMEM((b * nh, 128), F32),
            pltpu.VMEM((b // 4, nh, rows), F32),
            pltpu.VMEM((b, nqk), BF16),
            pltpu.VMEM((b, d), BF16),
            pltpu.VMEM((ndev, b, d), BF16),
            pltpu.VMEM((2 * TOP, 128), F32),
            pltpu.VMEM((ndev, 2 * TOP, 128), F32),
            pltpu.VMEM((t, 128), F32),
            DMA((RING,)), DMA((nk,)), DMA((nk,)), DMA((16,)),
            DMA((8,)), DMA((8,)), DMA((8,)), DMA((8,)), DMA((16,)), DMA((16,)),
        ],
        compiler_params=pltpu.CompilerParams(vmem_limit_bytes=63 * 2 ** 20, collective_id=0, has_side_effects=True),
        name="front",
    )(x, ln1.reshape(d // 128, 128), ln2.reshape(d // 128, 128), idx.T, gates.T, lens, wq, k, v, wo, ws1, ws3)


SMALL = 32


def _expert_kernel(big, u_hbm, key_ref, gsel_ref, krow, cnt, w1_hbm, w3_hbm, w2_hbm, p_ref,
                   u_v, w1_v, w3_v, w2_v, kcol, gcol, mid, order, u_sem, w_sem):
    t, d = u_v.shape
    ng = t // GROUP
    u_copy = pltpu.make_async_copy(u_hbm, u_v, u_sem)
    u_copy.start()
    for e in range(EDEV):
        n = cnt[0, e] + cnt[1, e]
        rank = 0
        for f in range(EDEV):
            if f != e:
                m = cnt[0, f] + cnt[1, f]
                rank += ((m >= n) if f < e else (m > n)).astype(jnp.int32)
        order[rank] = e

    def copy(i, hbm, vm, k):
        s = lax.rem(i, 2)
        return pltpu.make_async_copy(hbm.at[order[i]], vm.at[s], w_sem.at[s, k])

    def w1_copy(i):
        return copy(i, w1_hbm, w1_v, 0)

    def w3_copy(i):
        return copy(i, w3_hbm, w3_v, 1)

    def w2_copy(i):
        return copy(i, w2_hbm, w2_v, 2)

    for i in range(2):
        w1_copy(i).start()
        w3_copy(i).start()
        w2_copy(i).start()
    p_ref[...] = jnp.zeros_like(p_ref)
    for e in range(EDEV):
        kcol[e] = jnp.broadcast_to(key_ref[:, e:e + 1], (t, 128))
        gcol[e] = jnp.broadcast_to(gsel_ref[:, e:e + 1], (t, 128))
    u_copy.wait()

    def tokens(g):
        return pl.ds(g * GROUP if isinstance(g, int) else pl.multiple_of(g * GROUP, GROUP), GROUP)

    def pick(e, g, n):
        r = lax.broadcasted_iota(jnp.int32, (n, GROUP), 0).astype(F32)
        sel = jnp.where(krow[pl.ds(e, 1), tokens(g)] == r, 1.0, 0.0).astype(BF16)
        return jnp.dot(sel, u_v[tokens(g), :], preferred_element_type=F32).astype(BF16)

    def put(e, g, n, out):
        tl = tokens(g)
        r = lax.broadcasted_iota(jnp.int32, (GROUP, 128), 1).astype(F32)
        key = kcol[e, tl]
        sel = jnp.concatenate([jnp.where(key == r + 128.0 * q, 1.0, 0.0) for q in range(-(-n // 128))], axis=1)
        sel = sel[:, :n].astype(BF16)
        gt = gcol[e, tl]
        for q in range(d // 256):
            cs = slice(q * 256, (q + 1) * 256)
            back = jnp.dot(sel, out[:, cs], preferred_element_type=F32)
            p_ref[tl, cs] += back * jnp.concatenate([gt, gt], axis=1)

    def up(rows, s):
        return _silu_mul(jnp.dot(rows, w1_v[s], preferred_element_type=F32),
                         jnp.dot(rows, w3_v[s], preferred_element_type=F32))

    def down(g, s):
        return jnp.dot(g, w2_v[s], preferred_element_type=F32).astype(BF16)

    @pl.loop(0, EDEV)
    def _(i):
        e, s = order[i], lax.rem(i, 2)
        most = jnp.maximum(cnt[0, e], cnt[1, e])
        few = jnp.logical_and(most > 0, most <= SMALL)
        w1_copy(i).wait()
        w3_copy(i).wait()

        @pl.when(few)
        def _():
            rows = jnp.concatenate([pick(e, g, SMALL) for g in range(ng)], axis=0)
            mid[0:ng * SMALL, :] = up(rows, s)

        @pl.when(most > SMALL)
        def _():
            @pl.loop(0, ng)
            def _(g):
                mid[pl.ds(pl.multiple_of(g * GROUP, GROUP), big), :] = up(pick(e, g, big), s)

        @pl.when(i + 2 < EDEV)
        def _():
            w1_copy(i + 2).start()
            w3_copy(i + 2).start()

        w2_copy(i).wait()

        @pl.when(few)
        def _():
            out = down(mid[0:ng * SMALL, :], s)
            for g in range(ng):
                put(e, g, SMALL, out[g * SMALL:(g + 1) * SMALL])

        @pl.when(most > SMALL)
        def _():
            @pl.loop(0, ng)
            def _(g):
                put(e, g, big, down(mid[pl.ds(pl.multiple_of(g * GROUP, GROUP), big), :], s))

        @pl.when(i + 2 < EDEV)
        def _():
            w2_copy(i + 2).start()


def _experts(u, key, gsel, krow, cnt, w1, w3, w2, blk):
    t, d = u.shape
    f = w1.shape[2]
    cap = blk - blk // 8
    return pl.pallas_call(
        functools.partial(_expert_kernel, cap * (GROUP // blk)),
        out_shape=jax.ShapeDtypeStruct((t, d), F32),
        in_specs=[HBM, VMEM, VMEM, VMEM, SMEM, HBM, HBM, HBM],
        out_specs=VMEM,
        scratch_shapes=[
            pltpu.VMEM((t, d), BF16),
            pltpu.VMEM((2, d, f), BF16),
            pltpu.VMEM((2, d, f), BF16),
            pltpu.VMEM((2, f, d), BF16),
            pltpu.VMEM((EDEV, t, 128), F32),
            pltpu.VMEM((EDEV, t, 128), F32),
            pltpu.VMEM((t, f), BF16),
            pltpu.SMEM((EDEV,), jnp.int32),
            DMA(()), DMA((2, 3)),
        ],
        compiler_params=pltpu.CompilerParams(vmem_limit_bytes=56 * 2 ** 20),
        name="experts",
    )(u, key, gsel, krow, cnt, w1, w3, w2)


COLS = ((0, 640), (640, 640), (1280, 768))


def _combine_kernel(p_hbm, g_ref, h_ref, w_hbm, y_ref,
                    acc, r0, r1, r2, r3, w_v, sh, w_sem, p_sem,
                    s0, q0, s1, q1, s2, q2, s3, q3):
    z, y, x, c = _place()
    nw, _, wn = w_v.shape

    def w_copy(i):
        return pltpu.make_async_copy(w_hbm.at[:, pl.ds(i * wn, wn)], w_v.at[i], w_sem.at[i])

    streams = [(p, half) for half in range(2) for p in range(3)]
    place = {0: x, 1: y, 2: z}

    def cols(p):
        return pl.ds(COLS[p][0], COLS[p][1])

    def rows(half):
        return pl.ds(half * 16, 16)

    def load(k):
        p, half = streams[k]
        return pltpu.make_async_copy(p_hbm.at[:, :, :, c, rows(half), cols(p)], acc.at[:, :, :, rows(half), cols(p)],
                                     p_sem.at[k])

    def swap(k):
        p, half = streams[k]
        return pltpu.make_async_remote_copy(
            p_hbm.at[:, :, :, 1 - c, rows(half), cols(p)], r0.at[:, :, :, rows(half), cols(p)], s0.at[k], q0.at[k],
            device_id=_dev(z, y, x, 1 - c), device_id_type=MESH)

    def region(ref, p, half, step, mine):
        ix = [pl.ds(0, 2)] * 3
        for s in range(step):
            dim = (p + s) % 3
            v = place[dim]
            ix[2 - dim] = v if (s < step - 1 or mine) else 1 - v
        return ref.at[ix[0], ix[1], ix[2], rows(half), cols(p)]

    def landing(p, half, step):
        ref = (r1, r2, r3)[step - 1]
        if step == 1:
            return ref.at[:, :, rows(half), cols(p)]
        if step == 2:
            return ref.at[:, rows(half), cols(p)]
        return ref.at[rows(half), cols(p)]

    def hop(k, step):
        p, half = streams[k]
        dim = (p + step - 1) % 3
        o = [z, y, x]
        o[2 - dim] = 1 - o[2 - dim]
        send, recv = ((s1, q1), (s2, q2), (s3, q3))[step - 1]
        return pltpu.make_async_remote_copy(
            region(acc, p, half, step, False), landing(p, half, step), send.at[k], recv.at[k],
            device_id=_dev(*o, c), device_id_type=MESH)

    for k in range(6):
        load(k).start()
    barrier = pltpu.get_barrier_semaphore()
    pl.semaphore_signal(barrier, inc=1, device_id=_dev(z, y, x, 1 - c), device_id_type=MESH)
    for d in (1, 2, 4):
        pl.semaphore_signal(barrier, inc=1, device_id=_dev(*_offset((z, y, x), d), c), device_id_type=MESH)
    pl.semaphore_wait(barrier, 4)
    for k in range(6):
        swap(k).start()
    for i in range(nw):
        w_copy(i).start()

    def shared(i):
        w_copy(i).wait()
        cs = slice(i * wn, (i + 1) * wn)
        sh[:, cs] = jnp.dot(g_ref[...], w_v[i], preferred_element_type=F32) + h_ref[:, cs].astype(F32)

    for k in range(6):
        p, half = streams[k]
        load(k).wait()
        swap(k).wait_recv()
        rs, cs = slice(half * 16, half * 16 + 16), slice(COLS[p][0], COLS[p][0] + COLS[p][1])
        acc[:, :, :, rs, cs] += r0[:, :, :, rs, cs]
        hop(k, 1).start()
    shared(0)
    for k in range(6):
        p, half = streams[k]
        hop(k, 1).wait_recv()
        v = region(acc, p, half, 1, True)
        v[...] += landing(p, half, 1)[...]
        hop(k, 2).start()
    shared(1)
    shared(2)
    for k in range(6):
        p, half = streams[k]
        hop(k, 2).wait_recv()
        v = region(acc, p, half, 2, True)
        v[...] += landing(p, half, 2)[...]
        hop(k, 3).start()
    for i in range(3, nw):
        shared(i)
    for k in range(6):
        p, half = streams[k]
        hop(k, 3).wait_recv()
        v = region(acc, p, half, 3, True)
        tot = v[...] + landing(p, half, 3)[...]
        rs, cs = slice(half * 16, half * 16 + 16), slice(COLS[p][0], COLS[p][0] + COLS[p][1])
        y_ref[rs, cs] = (sh[rs, cs] + tot).astype(BF16)
    for k in range(6):
        swap(k).wait_send()
        for step in (1, 2, 3):
            hop(k, step).wait_send()


def _combine(part, g, h, ws2):
    b, d = h.shape
    fs = ws2.shape[0]
    nw = 8
    part = part.reshape(2, 2, 2, 2, b, d)
    return pl.pallas_call(
        _combine_kernel,
        out_shape=jax.ShapeDtypeStruct((b, d), BF16),
        in_specs=[HBM, VMEM, VMEM, HBM],
        out_specs=VMEM,
        scratch_shapes=[
            pltpu.VMEM((2, 2, 2, b, d), F32),
            pltpu.VMEM((2, 2, 2, b, d), F32),
            pltpu.VMEM((2, 2, b, d), F32),
            pltpu.VMEM((2, b, d), F32),
            pltpu.VMEM((b, d), F32),
            pltpu.VMEM((nw, fs, d // nw), BF16),
            pltpu.VMEM((b, d), F32),
            DMA((nw,)), DMA((6,)),
            DMA((6,)), DMA((6,)), DMA((6,)), DMA((6,)), DMA((6,)), DMA((6,)), DMA((6,)), DMA((6,)),
        ],
        compiler_params=pltpu.CompilerParams(vmem_limit_bytes=62 * 2 ** 20, collective_id=1, has_side_effects=True),
        name="combine",
    )(part, g, h, ws2)


def solution(mesh):
    def body(x, kv_k, kv_v, lens, idx, gates, ln1, wq, wo, ln2, ws1, ws3, ws2, w1, w3, w2):
        b, d = x.shape
        h, uall, g, key, gsel, krow, cnt = _front(x, kv_k, kv_v, lens, idx, gates, ln1, ln2, wq, wo, ws1, ws3)
        part = _experts(uall.reshape(16 * b, d), key, gsel, krow, cnt, w1, w3, w2, b)
        return _combine(part, g, h, ws2)

    rows = P(GRP)
    rep = P()
    return jax.shard_map(
        body, mesh=mesh,
        in_specs=(rows, rows, rows, rows, rows, rows, rep, rep, rep, rep, rep, rep, rep, rows, rows, rows),
        out_specs=rows, check_vma=False)
```

```python
import functools

import jax
import jax.numpy as jnp
from jax import lax
from jax.experimental import pallas as pl
from jax.experimental.pallas import tpu as pltpu
from jax.sharding import PartitionSpec as P

EPS = 1e-6
GRP = ("ey", "ex")
F32 = jnp.float32
BF16 = jnp.bfloat16
MESH = pl.DeviceIdType.MESH
VMEM = pl.BlockSpec(memory_space=pltpu.VMEM)
SMEM = pl.BlockSpec(memory_space=pltpu.SMEM)
HBM = pl.BlockSpec(memory_space=pltpu.HBM)
DMA = pltpu.SemaphoreType.DMA
TOP = 4
EDEV = 4


def _rms(v32, w):
    r = lax.rsqrt(jnp.mean(v32 * v32, axis=-1, keepdims=True) + EPS)
    return (v32 * r * w.astype(F32)).astype(BF16)


def _silu_mul(z1, z3):
    return (jax.nn.silu(z1) * z3).astype(BF16)


def _place():
    z = lax.axis_index("ey")
    ex = lax.axis_index("ex")
    return z, ex // 4, (ex // 2) % 2, ex % 2


def _dev(z, y, x, c):
    return (z, y * 4 + x * 2 + c)


def _flip(v, f):
    return 1 - v if f else v


def _offset(place, d):
    z, y, x = place
    return _flip(z, d // 4), _flip(y, (d // 2) % 2), _flip(x, d % 2)


CH = 512
RING = 18
GROUP = 256


def _front_kernel(cap, x_ref, ln1_ref, ln2_ref, idx_ref, gate_ref, lens_ref, wq_hbm, k_hbm, v_hbm, wo_hbm, ws1_hbm,
                  ws3_hbm, h_ref, hall_hbm, g_ref, key_ref, gsel_ref, krow_ref, cnt_ref,
                  ring, k_v, v_v, qs, sc, ob, us, ha, ms, ma, hit,
                  r_sem, k_sem, v_sem, out_sem, us_send, us_recv, uf_send, uf_recv, ms_send, ms_recv):
    b, d = x_ref.shape
    nqk = wq_hbm.shape[1]
    nh = nqk // 128
    nq = nqk // CH
    nk, kb, rows = k_v.shape[:3]
    nw = ws1_hbm.shape[1] // CH
    z, y, x, c = _place()
    me = ((z * 2 + y) * 2 + x) * 2 + c

    def cols(i):
        return pl.ds(i * CH if isinstance(i, int) else pl.multiple_of(i * CH, CH), CH)

    def chunk(src, n):
        s = lax.rem(n, RING)
        return pltpu.make_async_copy(src, ring.at[s], r_sem.at[s])

    def q_copy(i):
        return chunk(wq_hbm.at[:, cols(i)], i)

    def o_copy(i):
        return chunk(wo_hbm.at[pl.ds(pl.multiple_of((i % 2) * d, d), d), cols(i // 2)], nq + i)

    def w_copies(i):
        return chunk(ws1_hbm.at[:, cols(i)], 2 * nq + 2 * i), chunk(ws3_hbm.at[:, cols(i)], 2 * nq + 2 * i + 1)

    def k_copy(i):
        return pltpu.make_async_copy(k_hbm.at[i], k_v.at[i], k_sem.at[i])

    def v_copy(i):
        return pltpu.make_async_copy(v_hbm.at[i], v_v.at[i], v_sem.at[i])

    for i in range(nq):
        q_copy(i).start()
    barrier = pltpu.get_barrier_semaphore()
    peers = [_dev(*_offset((z, y, x), o % 8), _flip(c, o // 8)) for o in range(1, 16)]
    for dev in peers:
        pl.semaphore_signal(barrier, inc=1, device_id=dev, device_id_type=MESH)
    ms[...] = jnp.zeros_like(ms)
    ms[0:TOP, 0:b] = idx_ref[...].astype(F32)
    ms[TOP:2 * TOP, 0:b] = gate_ref[...]
    a = _rms(x_ref[...].astype(F32), _row(ln1_ref))

    @pl.loop(0, nq)
    def _(i):
        k_copy(i).start()
        v_copy(i).start()
        q_copy(i).wait()
        q = jnp.dot(a, ring[i], preferred_element_type=F32).astype(BF16).astype(F32)
        for j in range(CH // 128):
            qs[pl.ds(i * (CH // 128) + j, b, stride=nh), :] = q[:, j * 128:(j + 1) * 128]

    for i in range(2 * d // CH):
        o_copy(i).start()
    pl.semaphore_wait(barrier, 15)

    def m_send(o):
        return pltpu.make_async_remote_copy(ms, ma.at[me], ms_send.at[o], ms_recv.at[o], device_id=peers[o - 1],
                                            device_id_type=MESH)

    for o in range(1, 16):
        m_send(o).start()
    ma[me] = ms[...]

    kvh = 4
    row = lax.broadcasted_iota(jnp.int32, (nh, rows), 1)
    head = lax.broadcasted_iota(jnp.int32, (nh, rows), 0)
    pos = jnp.where(row % kvh == head // (nh // kvh), row // kvh, rows)

    def of(i):
        return pl.ds(pl.multiple_of(i * nh, nh), nh)

    @pl.loop(0, nk // 2)
    def _(i):
        for cp in w_copies(i):
            cp.start()
        for t in range(2):
            k_copy(i * 2 + t).wait()
            v_copy(i * 2 + t).wait()
        seqs = [(i * 2 + t, j, (i * 2 + t) * kb + j) for t in range(2) for j in range(kb)]
        for n, (ch, j, b_i) in enumerate(seqs):
            q = qs[of(b_i), :].astype(BF16)
            s = lax.dot_general(q, k_v[ch, j], (((1,), (1,)), ((), ())), preferred_element_type=F32) * 128 ** -0.5
            sc[n] = jnp.where(pos < lens_ref[b_i], s, -jnp.inf)
        ps = []
        for n in range(len(seqs)):
            s = sc[n]
            p = jnp.exp(s - jnp.max(s, axis=-1, keepdims=True))
            ps.append((p * (1.0 / jnp.sum(p, axis=-1, keepdims=True))).astype(BF16))
        for p, (ch, j, b_i) in zip(ps, seqs):
            qs[of(b_i), :] = jnp.dot(p, v_v[ch, j], preferred_element_type=F32)

    ahead = nk // 2
    while 2 * (ahead + 1) + nq <= RING:
        for cp in w_copies(ahead):
            cp.start()
        ahead += 1

    for hh in range(nh):
        ob[:, hh * 128:(hh + 1) * 128] = qs[pl.ds(hh, b, stride=nh), :].astype(BF16)

    no = d // CH

    def send(o, i):
        dev = _dev(*_offset((z, y, x), o), c) if o else _dev(z, y, x, 1 - c)
        return pltpu.make_async_remote_copy(h_ref.at[:, cols(i)], ha.at[me, :, cols(i)], us_send.at[o, i],
                                            us_recv.at[o, i], device_id=dev, device_id_type=MESH)

    def source(o, core):
        oz, oy, ox = _offset((z, y, x), o)
        return ((oz * 2 + oy) * 2 + ox) * 2 + core

    def forward(o, i):
        at = ha.at[source(o, c), :, cols(i)]
        return pltpu.make_async_remote_copy(at, at, uf_send.at[o, i], uf_recv.at[o, i],
                                            device_id=_dev(z, y, x, 1 - c), device_id_type=MESH)

    def store(o, core):
        src = source(o, core)
        return pltpu.make_async_copy(ha.at[src], hall_hbm.at[src], out_sem.at[2 * o + (0 if core is c else 1)])

    order = (7, 6, 5, 3, 4, 2, 1, 0)
    for i in range(no):
        acc = x_ref[:, cols(i)].astype(F32)
        attn = jnp.zeros((b, CH), F32)
        for t in range(2):
            o_copy(i * 2 + t).wait()
            attn += jnp.dot(ob[:, t * d:(t + 1) * d], ring[lax.rem(nq + i * 2 + t, RING)], preferred_element_type=F32)
        h_ref[:, cols(i)] = (acc + attn).astype(BF16)
        for cp in w_copies(ahead + i):
            cp.start()
        for o in order:
            send(o, i).start()

    ahead += no
    ha[me] = h_ref[...]
    us[...] = _rms(h_ref[...].astype(F32), _row(ln2_ref))

    def shared(i):
        c1, c3 = w_copies(i)
        c1.wait()
        c3.wait()
        s = lax.rem(2 * nq + 2 * i, RING)
        z1 = jnp.dot(us[...], ring[s], preferred_element_type=F32)
        z3 = jnp.dot(us[...], ring[s + 1], preferred_element_type=F32)
        g_ref[:, cols(i)] = _silu_mul(z1, z3)

    shared(0)

    n = 0
    while ahead < nw:
        for cp in w_copies(ahead):
            cp.start()
        ahead += 1
        n += 1
        if ahead < nw:
            shared(n)

    for o in range(1, 16):
        m_send(o).wait_recv()
    base = ((lax.axis_index("ey") * 8 + lax.axis_index("ex")) * EDEV).astype(F32)
    turned = ma[...].reshape(128, 128).T
    lane = lax.broadcasted_iota(jnp.int32, (b, 128), 1).astype(F32) + base
    nblk = ma.shape[0]
    for i in range(nblk):
        hb = jnp.zeros((b, 128), F32)
        gb = jnp.zeros((b, 128), F32)
        for j in range(TOP):
            at = i * 2 * TOP + j
            same = turned[0:b, at:at + 1] == lane
            hb += jnp.where(same, 1.0, 0.0)
            gb += jnp.where(same, turned[0:b, at + TOP:at + TOP + 1], 0.0)
        hit[i * b:(i + 1) * b, :] = hb
        gsel_ref[i * b:(i + 1) * b, :] = gb
    r0 = lax.broadcasted_iota(jnp.int32, (GROUP, GROUP), 0)
    r1 = lax.broadcasted_iota(jnp.int32, (GROUP, GROUP), 1)
    before = jnp.where(r1 < r0, 1.0, 0.0)
    before_blk = jnp.where(r1 // b == r0 // b, before, 0.0).astype(BF16)
    before = before.astype(BF16)
    for g in range(nblk * b // GROUP):
        sl = slice(g * GROUP, (g + 1) * GROUP)
        rank = jnp.dot(before_blk, hit[sl, :].astype(BF16), preferred_element_type=F32)
        keep = jnp.where(rank < cap, hit[sl, :], 0.0)
        at = jnp.dot(before, keep.astype(BF16), preferred_element_type=F32)
        key = jnp.where(keep > 0.0, at, -1.0)
        key_ref[sl, :] = key
        krow_ref[:, sl] = key.T[0:8]
        cnt_ref[g:g + 1, :] = jnp.sum(keep, axis=0, keepdims=True).astype(jnp.int32)

    for i in range(n if n else 1, nw):
        shared(i)
        at = {2: 0, 4: 1, 6: 2, 8: 3}.get(i)
        if at is not None:
            for o in order[:-1]:
                send(o, at).wait_recv()
                forward(o, at).start()
                if at == no - 1:
                    store(o, c).start()
            if at == no - 1:
                store(0, c).start()
                for t in range(no):
                    send(0, t).wait_recv()
                store(0, 1 - c).start()
    for o in order[:-1]:
        for t in range(no):
            forward(o, t).wait_recv()
        store(o, 1 - c).start()
    for o in range(8):
        for t in range(no):
            send(o, t).wait_send()
            if o:
                forward(o, t).wait_send()
        store(o, c).wait()
        store(o, 1 - c).wait()
    for o in range(1, 16):
        m_send(o).wait_send()


def _row(ref):
    return jnp.concatenate([ref[i:i + 1, :] for i in range(ref.shape[0])], axis=1)


def _front(x, k, v, lens, idx, gates, ln1, ln2, wq, wo, ws1, ws3):
    b, d = x.shape
    nqk, fs = wq.shape[1], ws1.shape[1]
    rows = k.shape[1] * k.shape[2]
    nk = 8
    ndev = 16
    k = k.reshape(nk, b // nk, rows, 128)
    v = v.reshape(nk, b // nk, rows, 128)
    nh = nqk // 128
    t = ndev * b
    return pl.pallas_call(
        functools.partial(_front_kernel, b - b // 8),
        out_shape=[jax.ShapeDtypeStruct((b, d), BF16), jax.ShapeDtypeStruct((ndev, b, d), BF16),
                   jax.ShapeDtypeStruct((b, fs), BF16), jax.ShapeDtypeStruct((t, 128), F32),
                   jax.ShapeDtypeStruct((t, 128), F32), jax.ShapeDtypeStruct((8, t), F32),
                   jax.ShapeDtypeStruct((t // GROUP, 128), jnp.int32)],
        in_specs=[VMEM] * 5 + [SMEM] + [HBM] * 6,
        out_specs=[VMEM, HBM] + [VMEM] * 5,
        scratch_shapes=[
            pltpu.VMEM((RING, d, CH), BF16),
            pltpu.VMEM((nk, b // nk, rows, 128), BF16),
            pltpu.VMEM((nk, b // nk, rows, 128), BF16),
            pltpu.VMEM((b * nh, 128), F32),
            pltpu.VMEM((b // 4, nh, rows), F32),
            pltpu.VMEM((b, nqk), BF16),
            pltpu.VMEM((b, d), BF16),
            pltpu.VMEM((ndev, b, d), BF16),
            pltpu.VMEM((2 * TOP, 128), F32),
            pltpu.VMEM((ndev, 2 * TOP, 128), F32),
            pltpu.VMEM((t, 128), F32),
            DMA((RING,)), DMA((nk,)), DMA((nk,)), DMA((16,)),
            DMA((8, d // CH)), DMA((8, d // CH)), DMA((8, d // CH)), DMA((8, d // CH)), DMA((16,)), DMA((16,)),
        ],
        compiler_params=pltpu.CompilerParams(vmem_limit_bytes=63 * 2 ** 20, collective_id=0, has_side_effects=True),
        name="front",
    )(x, ln1.reshape(d // 128, 128), ln2.reshape(d // 128, 128), idx.T, gates.T, lens, wq, k, v, wo, ws1, ws3)


SMALL = 32


def _expert_kernel(big, blk, h_hbm, ln2_ref, key_ref, gsel_ref, krow, cnt, w1_hbm, w3_hbm, w2_hbm, p_ref,
                   u_v, xs, zs, w1_v, w3_v, w2_v, kcol, gcol, mid, order, u_sem, w_sem):
    t, d = u_v.shape
    ng = t // GROUP
    u_copy = pltpu.make_async_copy(h_hbm, u_v, u_sem)
    u_copy.start()
    for e in range(EDEV):
        n = cnt[0, e] + cnt[1, e]
        rank = 0
        for f in range(EDEV):
            if f != e:
                m = cnt[0, f] + cnt[1, f]
                rank += ((m >= n) if f < e else (m > n)).astype(jnp.int32)
        order[rank] = e

    def copy(i, hbm, vm, k):
        s = lax.rem(i, 2)
        return pltpu.make_async_copy(hbm.at[order[i]], vm.at[s], w_sem.at[s, k])

    def w1_copy(i):
        return copy(i, w1_hbm, w1_v, 0)

    def w3_copy(i):
        return copy(i, w3_hbm, w3_v, 1)

    def w2_copy(i):
        return copy(i, w2_hbm, w2_v, 2)

    for i in range(2):
        w1_copy(i).start()
        w3_copy(i).start()
        w2_copy(i).start()
    p_ref[...] = jnp.zeros_like(p_ref)
    for e in range(EDEV):
        kcol[e] = jnp.broadcast_to(key_ref[:, e:e + 1], (t, 128))
        gcol[e] = jnp.broadcast_to(gsel_ref[:, e:e + 1], (t, 128))
    u_copy.wait()
    ln2 = _row(ln2_ref)

    @pl.loop(0, t // blk)
    def _(i):
        at = pl.ds(pl.multiple_of(i * blk, blk), blk)
        u_v[at, :] = _rms(u_v[at, :].astype(F32), ln2)

    def tokens(g):
        return pl.ds(g * GROUP if isinstance(g, int) else pl.multiple_of(g * GROUP, GROUP), GROUP)

    def pick(e, g, n):
        r = lax.broadcasted_iota(jnp.int32, (n, GROUP), 0).astype(F32)
        sel = jnp.where(krow[pl.ds(e, 1), tokens(g)] == r, 1.0, 0.0).astype(BF16)
        return jnp.dot(sel, u_v[tokens(g), :], preferred_element_type=F32).astype(BF16)

    def put(e, g, n, out):
        tl = tokens(g)
        r = lax.broadcasted_iota(jnp.int32, (GROUP, 128), 1).astype(F32)
        key = kcol[e, tl]
        sel = jnp.concatenate([jnp.where(key == r + 128.0 * q, 1.0, 0.0) for q in range(-(-n // 128))], axis=1)
        sel = sel[:, :n].astype(BF16)
        gt = gcol[e, tl]
        for q in range(d // 256):
            cs = slice(q * 256, (q + 1) * 256)
            back = jnp.dot(sel, out[:, cs], preferred_element_type=F32)
            p_ref[tl, cs] += back * jnp.concatenate([gt, gt], axis=1)

    def slots(g):
        return pl.ds(pl.multiple_of(g * big, 16), big)

    def down(g, s):
        return jnp.dot(g, w2_v[s], preferred_element_type=F32).astype(BF16)

    @pl.loop(0, EDEV)
    def _(i):
        e, s = order[i], lax.rem(i, 2)
        most = jnp.maximum(cnt[0, e], cnt[1, e])
        few = jnp.logical_and(most > 0, most <= SMALL)
        many = most > SMALL
        both = slice(0, ng * SMALL)

        @pl.when(few)
        def _():
            for g in range(ng):
                xs[g * SMALL:(g + 1) * SMALL, :] = pick(e, g, SMALL)

        @pl.when(many)
        def _():
            @pl.loop(0, ng)
            def _(g):
                xs[slots(g), :] = pick(e, g, big)

        w1_copy(i).wait()

        @pl.when(few)
        def _():
            zs[both, :] = jnp.dot(xs[both, :], w1_v[s], preferred_element_type=F32)

        @pl.when(many)
        def _():
            @pl.loop(0, ng)
            def _(g):
                zs[slots(g), :] = jnp.dot(xs[slots(g), :], w1_v[s], preferred_element_type=F32)

        @pl.when(i + 2 < EDEV)
        def _():
            w1_copy(i + 2).start()

        w3_copy(i).wait()

        @pl.when(few)
        def _():
            mid[both, :] = _silu_mul(zs[both, :], jnp.dot(xs[both, :], w3_v[s], preferred_element_type=F32))

        @pl.when(many)
        def _():
            @pl.loop(0, ng)
            def _(g):
                mid[slots(g), :] = _silu_mul(
                    zs[slots(g), :], jnp.dot(xs[slots(g), :], w3_v[s], preferred_element_type=F32))

        @pl.when(i + 2 < EDEV)
        def _():
            w3_copy(i + 2).start()

        w2_copy(i).wait()

        @pl.when(few)
        def _():
            out = down(mid[both, :], s)
            for g in range(ng):
                put(e, g, SMALL, out[g * SMALL:(g + 1) * SMALL])

        @pl.when(many)
        def _():
            @pl.loop(0, ng)
            def _(g):
                put(e, g, big, down(mid[slots(g), :], s))

        @pl.when(i + 2 < EDEV)
        def _():
            w2_copy(i + 2).start()


def _experts(h, ln2, key, gsel, krow, cnt, w1, w3, w2, blk):
    t, d = h.shape
    f = w1.shape[2]
    big = (blk - blk // 8) * (GROUP // blk)
    slots = big * (t // GROUP)
    return pl.pallas_call(
        functools.partial(_expert_kernel, big, blk),
        out_shape=jax.ShapeDtypeStruct((t, d), F32),
        in_specs=[HBM, VMEM, VMEM, VMEM, VMEM, SMEM, HBM, HBM, HBM],
        out_specs=VMEM,
        scratch_shapes=[
            pltpu.VMEM((t, d), BF16),
            pltpu.VMEM((slots, d), BF16),
            pltpu.VMEM((slots, f), F32),
            pltpu.VMEM((2, d, f), BF16),
            pltpu.VMEM((2, d, f), BF16),
            pltpu.VMEM((2, f, d), BF16),
            pltpu.VMEM((EDEV, t, 128), F32),
            pltpu.VMEM((EDEV, t, 128), F32),
            pltpu.VMEM((slots, f), BF16),
            pltpu.SMEM((EDEV,), jnp.int32),
            DMA(()), DMA((2, 3)),
        ],
        compiler_params=pltpu.CompilerParams(vmem_limit_bytes=58 * 2 ** 20),
        name="experts",
    )(h, ln2.reshape(d // 128, 128), key, gsel, krow, cnt, w1, w3, w2)


COLS = ((0, 640), (640, 640), (1280, 768))
PARTS, ROWS = 4, 8
NS = 3 * PARTS


def _combine_kernel(p_hbm, g_ref, h_ref, w_hbm, y_ref,
                    acc, r0, r1, r2, r3, w_v, sh, w_sem, p_sem,
                    s0, q0, s1, q1, s2, q2, s3, q3):
    z, y, x, c = _place()
    nw, _, wn = w_v.shape

    def w_copy(i):
        return pltpu.make_async_copy(w_hbm.at[:, pl.ds(i * wn, wn)], w_v.at[i], w_sem.at[i])

    streams = [(p, half) for half in range(PARTS) for p in range(3)]
    place = {0: x, 1: y, 2: z}

    def cols(p):
        return pl.ds(COLS[p][0], COLS[p][1])

    def rows(half):
        return pl.ds(half * ROWS, ROWS)

    def load(k):
        p, half = streams[k]
        return pltpu.make_async_copy(p_hbm.at[:, :, :, c, rows(half), cols(p)], acc.at[:, :, :, rows(half), cols(p)],
                                     p_sem.at[k])

    def swap(k):
        p, half = streams[k]
        return pltpu.make_async_remote_copy(
            p_hbm.at[:, :, :, 1 - c, rows(half), cols(p)], r0.at[:, :, :, rows(half), cols(p)], s0.at[k], q0.at[k],
            device_id=_dev(z, y, x, 1 - c), device_id_type=MESH)

    def region(ref, p, half, step, mine):
        ix = [pl.ds(0, 2)] * 3
        for s in range(step):
            dim = (p + s) % 3
            v = place[dim]
            ix[2 - dim] = v if (s < step - 1 or mine) else 1 - v
        return ref.at[ix[0], ix[1], ix[2], rows(half), cols(p)]

    def landing(p, half, step):
        ref = (r1, r2, r3)[step - 1]
        if step == 1:
            return ref.at[:, :, rows(half), cols(p)]
        if step == 2:
            return ref.at[:, rows(half), cols(p)]
        return ref.at[rows(half), cols(p)]

    def hop(k, step):
        p, half = streams[k]
        dim = (p + step - 1) % 3
        o = [z, y, x]
        o[2 - dim] = 1 - o[2 - dim]
        send, recv = ((s1, q1), (s2, q2), (s3, q3))[step - 1]
        return pltpu.make_async_remote_copy(
            region(acc, p, half, step, False), landing(p, half, step), send.at[k], recv.at[k],
            device_id=_dev(*o, c), device_id_type=MESH)

    for k in range(NS):
        load(k).start()
    barrier = pltpu.get_barrier_semaphore()
    pl.semaphore_signal(barrier, inc=1, device_id=_dev(z, y, x, 1 - c), device_id_type=MESH)
    for d in (1, 2, 4):
        pl.semaphore_signal(barrier, inc=1, device_id=_dev(*_offset((z, y, x), d), c), device_id_type=MESH)
    pl.semaphore_wait(barrier, 4)
    for k in range(NS):
        swap(k).start()
    for i in range(nw):
        w_copy(i).start()

    def shared(i):
        w_copy(i).wait()
        cs = slice(i * wn, (i + 1) * wn)
        sh[:, cs] = jnp.dot(g_ref[...], w_v[i], preferred_element_type=F32) + h_ref[:, cs].astype(F32)

    for k in range(NS):
        p, half = streams[k]
        load(k).wait()
        swap(k).wait_recv()
        rs, cs = slice(half * ROWS, half * ROWS + ROWS), slice(COLS[p][0], COLS[p][0] + COLS[p][1])
        acc[:, :, :, rs, cs] += r0[:, :, :, rs, cs]
        hop(k, 1).start()
    shared(0)
    for k in range(NS):
        p, half = streams[k]
        hop(k, 1).wait_recv()
        v = region(acc, p, half, 1, True)
        v[...] += landing(p, half, 1)[...]
        hop(k, 2).start()
    shared(1)
    shared(2)
    for k in range(NS):
        p, half = streams[k]
        hop(k, 2).wait_recv()
        v = region(acc, p, half, 2, True)
        v[...] += landing(p, half, 2)[...]
        hop(k, 3).start()
    for i in range(3, nw):
        shared(i)
    for k in range(NS):
        p, half = streams[k]
        hop(k, 3).wait_recv()
        v = region(acc, p, half, 3, True)
        tot = v[...] + landing(p, half, 3)[...]
        rs, cs = slice(half * ROWS, half * ROWS + ROWS), slice(COLS[p][0], COLS[p][0] + COLS[p][1])
        y_ref[rs, cs] = (sh[rs, cs] + tot).astype(BF16)
    for k in range(NS):
        swap(k).wait_send()
        for step in (1, 2, 3):
            hop(k, step).wait_send()


def _combine(part, g, h, ws2):
    b, d = h.shape
    fs = ws2.shape[0]
    nw = 8
    part = part.reshape(2, 2, 2, 2, b, d)
    return pl.pallas_call(
        _combine_kernel,
        out_shape=jax.ShapeDtypeStruct((b, d), BF16),
        in_specs=[HBM, VMEM, VMEM, HBM],
        out_specs=VMEM,
        scratch_shapes=[
            pltpu.VMEM((2, 2, 2, b, d), F32),
            pltpu.VMEM((2, 2, 2, b, d), F32),
            pltpu.VMEM((2, 2, b, d), F32),
            pltpu.VMEM((2, b, d), F32),
            pltpu.VMEM((b, d), F32),
            pltpu.VMEM((nw, fs, d // nw), BF16),
            pltpu.VMEM((b, d), F32),
            DMA((nw,)), DMA((NS,)),
            DMA((NS,)), DMA((NS,)), DMA((NS,)), DMA((NS,)), DMA((NS,)), DMA((NS,)), DMA((NS,)), DMA((NS,)),
        ],
        compiler_params=pltpu.CompilerParams(vmem_limit_bytes=62 * 2 ** 20, collective_id=1, has_side_effects=True),
        name="combine",
    )(part, g, h, ws2)


def solution(mesh):
    def body(x, kv_k, kv_v, lens, idx, gates, ln1, wq, wo, ln2, ws1, ws3, ws2, w1, w3, w2):
        b, d = x.shape
        h, hall, g, key, gsel, krow, cnt = _front(x, kv_k, kv_v, lens, idx, gates, ln1, ln2, wq, wo, ws1, ws3)
        part = _experts(hall.reshape(16 * b, d), ln2, key, gsel, krow, cnt, w1, w3, w2, b)
        return _combine(part, g, h, ws2)

    rows = P(GRP)
    rep = P()
    return jax.shard_map(
        body, mesh=mesh,
        in_specs=(rows, rows, rows, rows, rows, rows, rep, rep, rep, rep, rep, rep, rep, rows, rows, rows),
        out_specs=rows, check_vma=False)
```

```python
import functools

import jax
import jax.numpy as jnp
from jax import lax
from jax.experimental import pallas as pl
from jax.experimental.pallas import tpu as pltpu
from jax.sharding import PartitionSpec as P

EPS = 1e-6
GRP = ("ey", "ex")
F32 = jnp.float32
BF16 = jnp.bfloat16
MESH = pl.DeviceIdType.MESH
VMEM = pl.BlockSpec(memory_space=pltpu.VMEM)
SMEM = pl.BlockSpec(memory_space=pltpu.SMEM)
HBM = pl.BlockSpec(memory_space=pltpu.HBM)
DMA = pltpu.SemaphoreType.DMA
TOP = 4
EDEV = 4


def _rms(v32, w):
    r = lax.rsqrt(jnp.mean(v32 * v32, axis=-1, keepdims=True) + EPS)
    return (v32 * r * w.astype(F32)).astype(BF16)


def _silu_mul(z1, z3):
    return (jax.nn.silu(z1) * z3).astype(BF16)


def _place():
    z = lax.axis_index("ey")
    ex = lax.axis_index("ex")
    return z, ex // 4, (ex // 2) % 2, ex % 2


def _dev(z, y, x, c):
    return (z, y * 4 + x * 2 + c)


def _flip(v, f):
    return 1 - v if f else v


def _offset(place, d):
    z, y, x = place
    return _flip(z, d // 4), _flip(y, (d // 2) % 2), _flip(x, d % 2)


CH = 512
RING = 16
LATE = 3
GROUP = 256


def _front_kernel(cap, x_ref, ln1_ref, ln2_ref, idx_ref, gate_ref, lens_ref, wq_hbm, k_hbm, v_hbm, wo_hbm, ws1_hbm,
                  ws3_hbm, h_ref, us, uall_hbm, g_ref, key_ref, gsel_ref, krow_ref, cnt_ref,
                  ring, k_v, v_v, qs, sc, ob, ha, ua, ms, ma, hit,
                  r_sem, k_sem, v_sem, out_sem, us_send, us_recv, uf_send, uf_recv, ms_send, ms_recv):
    b, d = x_ref.shape
    nqk = wq_hbm.shape[1]
    nh = nqk // 128
    nq = nqk // CH
    nk, kb, rows = k_v.shape[:3]
    nw = ws1_hbm.shape[1] // CH - LATE
    z, y, x, c = _place()
    me = ((z * 2 + y) * 2 + x) * 2 + c

    def cols(i):
        return pl.ds(i * CH if isinstance(i, int) else pl.multiple_of(i * CH, CH), CH)

    def chunk(src, n):
        s = lax.rem(n, RING)
        return pltpu.make_async_copy(src, ring.at[s], r_sem.at[s])

    def q_copy(i):
        return chunk(wq_hbm.at[:, cols(i)], i)

    def o_copy(i):
        return chunk(wo_hbm.at[pl.ds(pl.multiple_of((i % 2) * d, d), d), cols(i // 2)], nq + i)

    def w_copies(i):
        return chunk(ws1_hbm.at[:, cols(i)], 2 * nq + 2 * i), chunk(ws3_hbm.at[:, cols(i)], 2 * nq + 2 * i + 1)

    def k_copy(i):
        return pltpu.make_async_copy(k_hbm.at[i], k_v.at[i], k_sem.at[i])

    def v_copy(i):
        return pltpu.make_async_copy(v_hbm.at[i], v_v.at[i], v_sem.at[i])

    for i in range(nq):
        q_copy(i).start()
    barrier = pltpu.get_barrier_semaphore()
    peers = [_dev(*_offset((z, y, x), o % 8), _flip(c, o // 8)) for o in range(1, 16)]
    for dev in peers:
        pl.semaphore_signal(barrier, inc=1, device_id=dev, device_id_type=MESH)
    ms[...] = jnp.zeros_like(ms)
    ms[0:TOP, 0:b] = idx_ref[...].astype(F32)
    ms[TOP:2 * TOP, 0:b] = gate_ref[...]
    a = _rms(x_ref[...].astype(F32), _row(ln1_ref))

    @pl.loop(0, nq)
    def _(i):
        k_copy(i).start()
        v_copy(i).start()
        q_copy(i).wait()
        q = jnp.dot(a, ring[i], preferred_element_type=F32).astype(BF16).astype(F32)
        for j in range(CH // 128):
            qs[pl.ds(i * (CH // 128) + j, b, stride=nh), :] = q[:, j * 128:(j + 1) * 128]

    for i in range(2 * d // CH):
        o_copy(i).start()
    pl.semaphore_wait(barrier, 15)

    def m_send(o):
        return pltpu.make_async_remote_copy(ms, ma.at[me], ms_send.at[o], ms_recv.at[o], device_id=peers[o - 1],
                                            device_id_type=MESH)

    for o in range(1, 16):
        m_send(o).start()
    ma[me] = ms[...]

    kvh = 4
    row = lax.broadcasted_iota(jnp.int32, (nh, rows), 1)
    head = lax.broadcasted_iota(jnp.int32, (nh, rows), 0)
    pos = jnp.where(row % kvh == head // (nh // kvh), row // kvh, rows)

    def of(i):
        return pl.ds(pl.multiple_of(i * nh, nh), nh)

    @pl.loop(0, nk // 2)
    def _(i):
        for cp in w_copies(i):
            cp.start()
        for t in range(2):
            k_copy(i * 2 + t).wait()
            v_copy(i * 2 + t).wait()
        seqs = [(i * 2 + t, j, (i * 2 + t) * kb + j) for t in range(2) for j in range(kb)]
        for n, (ch, j, b_i) in enumerate(seqs):
            q = qs[of(b_i), :].astype(BF16)
            s = lax.dot_general(q, k_v[ch, j], (((1,), (1,)), ((), ())), preferred_element_type=F32) * 128 ** -0.5
            sc[n] = jnp.where(pos < lens_ref[b_i], s, -jnp.inf)
        ps = []
        for n in range(len(seqs)):
            s = sc[n]
            p = jnp.exp(s - jnp.max(s, axis=-1, keepdims=True))
            ps.append((p * (1.0 / jnp.sum(p, axis=-1, keepdims=True))).astype(BF16))
        for p, (ch, j, b_i) in zip(ps, seqs):
            qs[of(b_i), :] = jnp.dot(p, v_v[ch, j], preferred_element_type=F32)

    ahead = nk // 2
    while 2 * (ahead + 1) + nq <= RING:
        for cp in w_copies(ahead):
            cp.start()
        ahead += 1

    for hh in range(nh):
        ob[:, hh * 128:(hh + 1) * 128] = qs[pl.ds(hh, b, stride=nh), :].astype(BF16)

    no = d // CH

    def send(o, i):
        dev = _dev(*_offset((z, y, x), o), c) if o else _dev(z, y, x, 1 - c)
        return pltpu.make_async_remote_copy(h_ref.at[:, cols(i)], ha.at[me, :, cols(i)], us_send.at[o, i],
                                            us_recv.at[o, i], device_id=dev, device_id_type=MESH)

    def source(o, core):
        oz, oy, ox = _offset((z, y, x), o)
        return ((oz * 2 + oy) * 2 + ox) * 2 + core

    def forward(o, i):
        at = ha.at[source(o, c), :, cols(i)]
        return pltpu.make_async_remote_copy(at, at, uf_send.at[o, i], uf_recv.at[o, i],
                                            device_id=_dev(z, y, x, 1 - c), device_id_type=MESH)

    def store(o, core):
        src = source(o, core)
        return pltpu.make_async_copy(ua.at[src], uall_hbm.at[src], out_sem.at[2 * o + (0 if core is c else 1)])

    order = (7, 6, 5, 3, 4, 2, 1, 0)
    for i in range(no):
        acc = x_ref[:, cols(i)].astype(F32)
        attn = jnp.zeros((b, CH), F32)
        for t in range(2):
            o_copy(i * 2 + t).wait()
            attn += jnp.dot(ob[:, t * d:(t + 1) * d], ring[lax.rem(nq + i * 2 + t, RING)], preferred_element_type=F32)
        h_ref[:, cols(i)] = (acc + attn).astype(BF16)
        for cp in w_copies(ahead + i):
            cp.start()
        for o in order:
            send(o, i).start()

    ahead += no
    ln2 = _row(ln2_ref)
    us[...] = _rms(h_ref[...].astype(F32), ln2)

    def shared(i):
        c1, c3 = w_copies(i)
        c1.wait()
        c3.wait()
        s = lax.rem(2 * nq + 2 * i, RING)
        z1 = jnp.dot(us[...], ring[s], preferred_element_type=F32)
        z3 = jnp.dot(us[...], ring[s + 1], preferred_element_type=F32)
        g_ref[:, cols(i)] = _silu_mul(z1, z3)

    ua[me] = us[...]
    shared(0)

    n = 0
    while ahead < nw:
        for cp in w_copies(ahead):
            cp.start()
        ahead += 1
        n += 1
        if ahead < nw:
            shared(n)

    for o in range(1, 16):
        m_send(o).wait_recv()
    base = ((lax.axis_index("ey") * 8 + lax.axis_index("ex")) * EDEV).astype(F32)
    turned = ma[...].reshape(128, 128).T
    lane = lax.broadcasted_iota(jnp.int32, (b, 128), 1).astype(F32) + base
    nblk = ma.shape[0]
    for i in range(nblk):
        hb = jnp.zeros((b, 128), F32)
        gb = jnp.zeros((b, 128), F32)
        for j in range(TOP):
            at = i * 2 * TOP + j
            same = turned[0:b, at:at + 1] == lane
            hb += jnp.where(same, 1.0, 0.0)
            gb += jnp.where(same, turned[0:b, at + TOP:at + TOP + 1], 0.0)
        hit[i * b:(i + 1) * b, :] = hb
        gsel_ref[i * b:(i + 1) * b, :] = gb
    r0 = lax.broadcasted_iota(jnp.int32, (GROUP, GROUP), 0)
    r1 = lax.broadcasted_iota(jnp.int32, (GROUP, GROUP), 1)
    before = jnp.where(r1 < r0, 1.0, 0.0)
    before_blk = jnp.where(r1 // b == r0 // b, before, 0.0).astype(BF16)
    before = before.astype(BF16)
    for g in range(nblk * b // GROUP):
        sl = slice(g * GROUP, (g + 1) * GROUP)
        rank = jnp.dot(before_blk, hit[sl, :].astype(BF16), preferred_element_type=F32)
        keep = jnp.where(rank < cap, hit[sl, :], 0.0)
        at = jnp.dot(before, keep.astype(BF16), preferred_element_type=F32)
        key = jnp.where(keep > 0.0, at, -1.0)
        key_ref[sl, :] = key
        krow_ref[:, sl] = key.T[0:8]
        cnt_ref[g:g + 1, :] = jnp.sum(keep, axis=0, keepdims=True).astype(jnp.int32)

    for i in range(n if n else 1, nw):
        shared(i)
        at = {1: 0, 3: 1, 5: 2, 7: 3}.get(i)
        if at is not None:
            for o in order[:-1]:
                send(o, at).wait_recv()
                forward(o, at).start()

    def normalise(o, core):
        src = source(o, core)
        ua[src] = _rms(ha[src].astype(F32), ln2)

    for o in order[:-1]:
        normalise(o, c)
    for o in range(8):
        store(o, c).start()
    for t in range(no):
        send(0, t).wait_recv()
    for o in order[:-1]:
        for t in range(no):
            forward(o, t).wait_recv()
    for o in range(8):
        normalise(o, 1 - c)
    for o in range(8):
        store(o, 1 - c).start()
    for o in range(8):
        for t in range(no):
            send(o, t).wait_send()
            if o:
                forward(o, t).wait_send()
        store(o, c).wait()
        store(o, 1 - c).wait()
    for o in range(1, 16):
        m_send(o).wait_send()


def _row(ref):
    return jnp.concatenate([ref[i:i + 1, :] for i in range(ref.shape[0])], axis=1)


def _front(x, k, v, lens, idx, gates, ln1, ln2, wq, wo, ws1, ws3):
    b, d = x.shape
    nqk, fs = wq.shape[1], ws1.shape[1] - LATE * CH
    rows = k.shape[1] * k.shape[2]
    nk = 8
    ndev = 16
    k = k.reshape(nk, b // nk, rows, 128)
    v = v.reshape(nk, b // nk, rows, 128)
    nh = nqk // 128
    t = ndev * b
    return pl.pallas_call(
        functools.partial(_front_kernel, b - b // 8),
        out_shape=[jax.ShapeDtypeStruct((b, d), BF16)] * 2 + [jax.ShapeDtypeStruct((ndev, b, d), BF16),
                   jax.ShapeDtypeStruct((b, fs), BF16), jax.ShapeDtypeStruct((t, 128), F32),
                   jax.ShapeDtypeStruct((t, 128), F32), jax.ShapeDtypeStruct((8, t), F32),
                   jax.ShapeDtypeStruct((t // GROUP, 128), jnp.int32)],
        in_specs=[VMEM] * 5 + [SMEM] + [HBM] * 6,
        out_specs=[VMEM, VMEM, HBM] + [VMEM] * 5,
        scratch_shapes=[
            pltpu.VMEM((RING, d, CH), BF16),
            pltpu.VMEM((nk, b // nk, rows, 128), BF16),
            pltpu.VMEM((nk, b // nk, rows, 128), BF16),
            pltpu.VMEM((b * nh, 128), F32),
            pltpu.VMEM((b // 4, nh, rows), F32),
            pltpu.VMEM((b, nqk), BF16),
            pltpu.VMEM((ndev, b, d), BF16),
            pltpu.VMEM((ndev, b, d), BF16),
            pltpu.VMEM((2 * TOP, 128), F32),
            pltpu.VMEM((ndev, 2 * TOP, 128), F32),
            pltpu.VMEM((t, 128), F32),
            DMA((RING,)), DMA((nk,)), DMA((nk,)), DMA((16,)),
            DMA((8, d // CH)), DMA((8, d // CH)), DMA((8, d // CH)), DMA((8, d // CH)), DMA((16,)), DMA((16,)),
        ],
        compiler_params=pltpu.CompilerParams(vmem_limit_bytes=63 * 2 ** 20, collective_id=0, has_side_effects=True),
        name="front",
    )(x, ln1.reshape(d // 128, 128), ln2.reshape(d // 128, 128), idx.T, gates.T, lens, wq, k, v, wo, ws1, ws3)


SMALL = 32


def _expert_kernel(big, u_hbm, key_ref, gsel_ref, krow, cnt, w1_hbm, w3_hbm, w2_hbm, p_ref,
                   u_v, xs, zs, w1_v, w3_v, w2_v, mid, order, u_sem, w_sem):
    t, d = u_v.shape
    ng = t // GROUP
    u_copy = pltpu.make_async_copy(u_hbm, u_v, u_sem)
    u_copy.start()
    for e in range(EDEV):
        n = cnt[0, e] + cnt[1, e]
        rank = 0
        for f in range(EDEV):
            if f != e:
                m = cnt[0, f] + cnt[1, f]
                rank += ((m >= n) if f < e else (m > n)).astype(jnp.int32)
        order[rank] = e

    def copy(i, hbm, vm, k):
        s = lax.rem(i, 2)
        return pltpu.make_async_copy(hbm.at[order[i]], vm.at[s], w_sem.at[s, k])

    def w1_copy(i):
        return copy(i, w1_hbm, w1_v, 0)

    def w3_copy(i):
        return copy(i, w3_hbm, w3_v, 1)

    def w2_copy(i):
        return copy(i, w2_hbm, w2_v, 2)

    for i in range(2):
        w1_copy(i).start()
        w3_copy(i).start()
        w2_copy(i).start()
    p_ref[...] = jnp.zeros_like(p_ref)
    u_copy.wait()
    lane = lax.broadcasted_iota(jnp.int32, (GROUP, 128), 1)

    def tokens(g):
        return pl.ds(g * GROUP if isinstance(g, int) else pl.multiple_of(g * GROUP, GROUP), GROUP)

    def pick(e, g, n):
        r = lax.broadcasted_iota(jnp.int32, (n, GROUP), 0).astype(F32)
        sel = jnp.where(krow[pl.ds(e, 1), tokens(g)] == r, 1.0, 0.0).astype(BF16)
        return jnp.dot(sel, u_v[tokens(g), :], preferred_element_type=F32).astype(BF16)

    def put(e, g, n, out):
        tl = tokens(g)
        r = lax.broadcasted_iota(jnp.int32, (GROUP, 128), 1).astype(F32)
        key = jnp.sum(jnp.where(lane == e, key_ref[tl, :], 0.0), axis=1, keepdims=True)
        sel = jnp.concatenate([jnp.where(key == r + 128.0 * q, 1.0, 0.0) for q in range(-(-n // 128))], axis=1)
        sel = sel[:, :n].astype(BF16)
        gt = jnp.sum(jnp.where(lane == e, gsel_ref[tl, :], 0.0), axis=1, keepdims=True)
        for q in range(d // 256):
            cs = slice(q * 256, (q + 1) * 256)
            back = jnp.dot(sel, out[:, cs], preferred_element_type=F32)
            p_ref[tl, cs] += back * gt

    def slots(g):
        return pl.ds(pl.multiple_of(g * big, 16), big)

    def down(g, s):
        return jnp.dot(g, w2_v[s], preferred_element_type=F32).astype(BF16)

    @pl.loop(0, EDEV)
    def _(i):
        e, s = order[i], lax.rem(i, 2)
        most = jnp.maximum(cnt[0, e], cnt[1, e])
        few = jnp.logical_and(most > 0, most <= SMALL)
        many = most > SMALL
        both = slice(0, ng * SMALL)

        @pl.when(few)
        def _():
            for g in range(ng):
                xs[g * SMALL:(g + 1) * SMALL, :] = pick(e, g, SMALL)

        @pl.when(many)
        def _():
            @pl.loop(0, ng)
            def _(g):
                xs[slots(g), :] = pick(e, g, big)

        w1_copy(i).wait()

        @pl.when(few)
        def _():
            zs[both, :] = jnp.dot(xs[both, :], w1_v[s], preferred_element_type=F32)

        @pl.when(many)
        def _():
            @pl.loop(0, ng)
            def _(g):
                zs[slots(g), :] = jnp.dot(xs[slots(g), :], w1_v[s], preferred_element_type=F32)

        @pl.when(i + 2 < EDEV)
        def _():
            w1_copy(i + 2).start()

        w3_copy(i).wait()

        @pl.when(few)
        def _():
            mid[both, :] = _silu_mul(zs[both, :], jnp.dot(xs[both, :], w3_v[s], preferred_element_type=F32))

        @pl.when(many)
        def _():
            @pl.loop(0, ng)
            def _(g):
                mid[slots(g), :] = _silu_mul(
                    zs[slots(g), :], jnp.dot(xs[slots(g), :], w3_v[s], preferred_element_type=F32))

        @pl.when(i + 2 < EDEV)
        def _():
            w3_copy(i + 2).start()

        w2_copy(i).wait()

        @pl.when(few)
        def _():
            out = down(mid[both, :], s)
            for g in range(ng):
                put(e, g, SMALL, out[g * SMALL:(g + 1) * SMALL])

        @pl.when(many)
        def _():
            @pl.loop(0, ng)
            def _(g):
                put(e, g, big, down(mid[slots(g), :], s))

        @pl.when(i + 2 < EDEV)
        def _():
            w2_copy(i + 2).start()


def _experts(u, key, gsel, krow, cnt, w1, w3, w2, blk):
    t, d = u.shape
    f = w1.shape[2]
    big = (blk - blk // 8) * (GROUP // blk)
    slots = big * (t // GROUP)
    return pl.pallas_call(
        functools.partial(_expert_kernel, big),
        out_shape=jax.ShapeDtypeStruct((t, d), F32),
        in_specs=[HBM, VMEM, VMEM, VMEM, SMEM, HBM, HBM, HBM],
        out_specs=VMEM,
        scratch_shapes=[
            pltpu.VMEM((t, d), BF16),
            pltpu.VMEM((slots, d), BF16),
            pltpu.VMEM((slots, f), F32),
            pltpu.VMEM((2, d, f), BF16),
            pltpu.VMEM((2, d, f), BF16),
            pltpu.VMEM((2, f, d), BF16),
            pltpu.VMEM((slots, f), BF16),
            pltpu.SMEM((EDEV,), jnp.int32),
            DMA(()), DMA((2, 3)),
        ],
        compiler_params=pltpu.CompilerParams(vmem_limit_bytes=55 * 2 ** 20),
        name="experts",
    )(u, key, gsel, krow, cnt, w1, w3, w2)


COLS = ((0, 640), (640, 640), (1280, 768))
PARTS, ROWS = 4, 8
NS = 3 * PARTS


def _combine_kernel(p_ref, g_ref, h_ref, u_ref, ws1_hbm, ws3_hbm, w_hbm, y_ref,
                    acc, r0, r1, r2, r3, w_v, a_v, b_v, late, sh, w_sem, a_sem, b_sem,
                    s0, q0, s1, q1, s2, q2, s3, q3):
    z, y, x, c = _place()
    nw, _, wn = w_v.shape

    def w_copy(i):
        return pltpu.make_async_copy(w_hbm.at[:, pl.ds(i * wn, wn)], w_v.at[i], w_sem.at[i])

    streams = [(p, half) for half in range(PARTS) for p in range(3)]
    place = {0: x, 1: y, 2: z}

    def cols(p):
        return pl.ds(COLS[p][0], COLS[p][1])

    def rows(half):
        return pl.ds(half * ROWS, ROWS)

    early = g_ref.shape[1]

    def a_copy(i):
        return pltpu.make_async_copy(ws1_hbm.at[:, pl.ds(early + i * CH, CH)], a_v.at[i], a_sem.at[i])

    def b_copy(i):
        return pltpu.make_async_copy(ws3_hbm.at[:, pl.ds(early + i * CH, CH)], b_v.at[i], b_sem.at[i])

    def swap(k):
        p, half = streams[k]
        return pltpu.make_async_remote_copy(
            p_ref.at[:, :, :, 1 - c, rows(half), cols(p)], r0.at[:, :, :, rows(half), cols(p)], s0.at[k], q0.at[k],
            device_id=_dev(z, y, x, 1 - c), device_id_type=MESH)

    def region(ref, p, half, step, mine):
        ix = [pl.ds(0, 2)] * 3
        for s in range(step):
            dim = (p + s) % 3
            v = place[dim]
            ix[2 - dim] = v if (s < step - 1 or mine) else 1 - v
        return ref.at[ix[0], ix[1], ix[2], rows(half), cols(p)]

    def landing(p, half, step):
        ref = (r1, r2, r3)[step - 1]
        if step == 1:
            return ref.at[:, :, rows(half), cols(p)]
        if step == 2:
            return ref.at[:, rows(half), cols(p)]
        return ref.at[rows(half), cols(p)]

    def hop(k, step):
        p, half = streams[k]
        dim = (p + step - 1) % 3
        o = [z, y, x]
        o[2 - dim] = 1 - o[2 - dim]
        send, recv = ((s1, q1), (s2, q2), (s3, q3))[step - 1]
        return pltpu.make_async_remote_copy(
            region(acc, p, half, step, False), landing(p, half, step), send.at[k], recv.at[k],
            device_id=_dev(*o, c), device_id_type=MESH)

    for i in range(LATE):
        a_copy(i).start()
        b_copy(i).start()
    barrier = pltpu.get_barrier_semaphore()
    pl.semaphore_signal(barrier, inc=1, device_id=_dev(z, y, x, 1 - c), device_id_type=MESH)
    for d in (1, 2, 4):
        pl.semaphore_signal(barrier, inc=1, device_id=_dev(*_offset((z, y, x), d), c), device_id_type=MESH)
    pl.semaphore_wait(barrier, 4)
    for k in range(NS):
        swap(k).start()
    for i in range(nw):
        w_copy(i).start()

    def shared(i):
        w_copy(i).wait()
        cs = slice(i * wn, (i + 1) * wn)
        s = jnp.dot(g_ref[...], w_v[i, 0:early], preferred_element_type=F32)
        s += jnp.dot(late[...], w_v[i, early:], preferred_element_type=F32)
        sh[:, cs] = s + h_ref[:, cs].astype(F32)

    def up(i):
        a_copy(i).wait()
        b_copy(i).wait()
        late[:, i * CH:(i + 1) * CH] = _silu_mul(jnp.dot(u_ref[...], a_v[i], preferred_element_type=F32),
                                                 jnp.dot(u_ref[...], b_v[i], preferred_element_type=F32))

    for k in range(NS):
        p, half = streams[k]
        swap(k).wait_recv()
        rs, cs = slice(half * ROWS, half * ROWS + ROWS), slice(COLS[p][0], COLS[p][0] + COLS[p][1])
        acc[:, :, :, rs, cs] = p_ref[:, :, :, c, rs, cs] + r0[:, :, :, rs, cs]
        hop(k, 1).start()
    for i in range(LATE):
        up(i)
    for k in range(NS):
        p, half = streams[k]
        hop(k, 1).wait_recv()
        v = region(acc, p, half, 1, True)
        v[...] += landing(p, half, 1)[...]
        hop(k, 2).start()
    for i in range(3):
        shared(i)
    for k in range(NS):
        p, half = streams[k]
        hop(k, 2).wait_recv()
        v = region(acc, p, half, 2, True)
        v[...] += landing(p, half, 2)[...]
        hop(k, 3).start()
    for i in range(3, nw):
        shared(i)
    for k in range(NS):
        p, half = streams[k]
        hop(k, 3).wait_recv()
        v = region(acc, p, half, 3, True)
        tot = v[...] + landing(p, half, 3)[...]
        rs, cs = slice(half * ROWS, half * ROWS + ROWS), slice(COLS[p][0], COLS[p][0] + COLS[p][1])
        y_ref[rs, cs] = (sh[rs, cs] + tot).astype(BF16)
    for k in range(NS):
        swap(k).wait_send()
        for step in (1, 2, 3):
            hop(k, step).wait_send()


def _combine(part, g, h, u, ws1, ws3, ws2):
    b, d = h.shape
    fs = ws2.shape[0]
    nw = 8
    part = part.reshape(2, 2, 2, 2, b, d)
    return pl.pallas_call(
        _combine_kernel,
        out_shape=jax.ShapeDtypeStruct((b, d), BF16),
        in_specs=[VMEM, VMEM, VMEM, VMEM, HBM, HBM, HBM],
        out_specs=VMEM,
        scratch_shapes=[
            pltpu.VMEM((2, 2, 2, b, d), F32),
            pltpu.VMEM((2, 2, 2, b, d), F32),
            pltpu.VMEM((2, 2, b, d), F32),
            pltpu.VMEM((2, b, d), F32),
            pltpu.VMEM((b, d), F32),
            pltpu.VMEM((nw, fs, d // nw), BF16),
            pltpu.VMEM((LATE, d, CH), BF16),
            pltpu.VMEM((LATE, d, CH), BF16),
            pltpu.VMEM((b, LATE * CH), BF16),
            pltpu.VMEM((b, d), F32),
            DMA((nw,)), DMA((LATE,)), DMA((LATE,)),
            DMA((NS,)), DMA((NS,)), DMA((NS,)), DMA((NS,)), DMA((NS,)), DMA((NS,)), DMA((NS,)), DMA((NS,)),
        ],
        compiler_params=pltpu.CompilerParams(vmem_limit_bytes=52 * 2 ** 20, collective_id=1, has_side_effects=True),
        name="combine",
    )(part, g, h, u, ws1, ws3, ws2)


def solution(mesh):
    def body(x, kv_k, kv_v, lens, idx, gates, ln1, wq, wo, ln2, ws1, ws3, ws2, w1, w3, w2):
        b, d = x.shape
        h, u, uall, g, key, gsel, krow, cnt = _front(x, kv_k, kv_v, lens, idx, gates, ln1, ln2, wq, wo, ws1, ws3)
        part = _experts(uall.reshape(16 * b, d), key, gsel, krow, cnt, w1, w3, w2, b)
        return _combine(part, g, h, u, ws1, ws3, ws2)

    rows = P(GRP)
    rep = P()
    return jax.shard_map(
        body, mesh=mesh,
        in_specs=(rows, rows, rows, rows, rows, rows, rep, rep, rep, rep, rep, rep, rep, rows, rows, rows),
        out_specs=rows, check_vma=False)
```

```python
import functools

import jax
import jax.numpy as jnp
from jax import lax
from jax.experimental import pallas as pl
from jax.experimental.pallas import tpu as pltpu
from jax.sharding import PartitionSpec as P

EPS = 1e-6
GRP = ("ey", "ex")
F32 = jnp.float32
BF16 = jnp.bfloat16
MESH = pl.DeviceIdType.MESH
VMEM = pl.BlockSpec(memory_space=pltpu.VMEM)
SMEM = pl.BlockSpec(memory_space=pltpu.SMEM)
HBM = pl.BlockSpec(memory_space=pltpu.HBM)
DMA = pltpu.SemaphoreType.DMA
TOP = 4
EDEV = 4


def _rms(v32, w):
    r = lax.rsqrt(jnp.mean(v32 * v32, axis=-1, keepdims=True) + EPS)
    return (v32 * r * w.astype(F32)).astype(BF16)


def _silu_mul(z1, z3):
    return (jax.nn.silu(z1) * z3).astype(BF16)


def _place():
    z = lax.axis_index("ey")
    ex = lax.axis_index("ex")
    return z, ex // 4, (ex // 2) % 2, ex % 2


def _dev(z, y, x, c):
    return (z, y * 4 + x * 2 + c)


def _flip(v, f):
    return 1 - v if f else v


def _offset(place, d):
    z, y, x = place
    return _flip(z, d // 4), _flip(y, (d // 2) % 2), _flip(x, d % 2)


CH = 512
RING = 16
LATE = 3
GROUP = 256


def _front_kernel(cap, x_ref, ln1_ref, ln2_ref, idx_ref, gate_ref, lens_ref, wq_hbm, k_hbm, v_hbm, wo_hbm, ws1_hbm,
                  ws3_hbm, h_ref, us, uall_hbm, g_ref, key_ref, gsel_ref, krow_ref, cnt_ref,
                  ring, k_v, v_v, qs, sc, ob, ha, ua, ms, ma, hit,
                  r_sem, k_sem, v_sem, out_sem, us_send, us_recv, uf_send, uf_recv, ms_send, ms_recv):
    b, d = x_ref.shape
    nqk = wq_hbm.shape[1]
    nh = nqk // 128
    nq = nqk // CH
    nk, kb, rows = k_v.shape[:3]
    nw = ws1_hbm.shape[1] // CH - LATE
    z, y, x, c = _place()
    me = ((z * 2 + y) * 2 + x) * 2 + c

    def cols(i):
        return pl.ds(i * CH if isinstance(i, int) else pl.multiple_of(i * CH, CH), CH)

    def chunk(src, n):
        s = lax.rem(n, RING)
        return pltpu.make_async_copy(src, ring.at[s], r_sem.at[s])

    def q_copy(i):
        return chunk(wq_hbm.at[:, cols(i)], i)

    def o_copy(i):
        return chunk(wo_hbm.at[pl.ds(pl.multiple_of((i % 2) * d, d), d), cols(i // 2)], nq + i)

    def w_copies(i):
        return chunk(ws1_hbm.at[:, cols(i)], 2 * nq + 2 * i), chunk(ws3_hbm.at[:, cols(i)], 2 * nq + 2 * i + 1)

    def k_copy(i):
        return pltpu.make_async_copy(k_hbm.at[i], k_v.at[i], k_sem.at[i])

    def v_copy(i):
        return pltpu.make_async_copy(v_hbm.at[i], v_v.at[i], v_sem.at[i])

    for i in range(nq):
        q_copy(i).start()
    barrier = pltpu.get_barrier_semaphore()
    peers = [_dev(*_offset((z, y, x), o % 8), _flip(c, o // 8)) for o in range(1, 16)]
    for dev in peers:
        pl.semaphore_signal(barrier, inc=1, device_id=dev, device_id_type=MESH)
    ms[...] = jnp.zeros_like(ms)
    ms[0:TOP, 0:b] = idx_ref[...].astype(F32)
    ms[TOP:2 * TOP, 0:b] = gate_ref[...]
    a = _rms(x_ref[...].astype(F32), _row(ln1_ref))

    @pl.loop(0, nq)
    def _(i):
        k_copy(i).start()
        v_copy(i).start()
        q_copy(i).wait()
        q = jnp.dot(a, ring[i], preferred_element_type=F32).astype(BF16).astype(F32)
        for j in range(CH // 128):
            qs[pl.ds(i * (CH // 128) + j, b, stride=nh), :] = q[:, j * 128:(j + 1) * 128]

    for i in range(2 * d // CH):
        o_copy(i).start()
    pl.semaphore_wait(barrier, 15)

    def m_send(o):
        return pltpu.make_async_remote_copy(ms, ma.at[me], ms_send.at[o], ms_recv.at[o], device_id=peers[o - 1],
                                            device_id_type=MESH)

    for o in range(1, 16):
        m_send(o).start()
    ma[me] = ms[...]

    kvh = 4
    row = lax.broadcasted_iota(jnp.int32, (nh, rows), 1)
    head = lax.broadcasted_iota(jnp.int32, (nh, rows), 0)
    pos = jnp.where(row % kvh == head // (nh // kvh), row // kvh, rows)

    def of(i):
        return pl.ds(pl.multiple_of(i * nh, nh), nh)

    @pl.loop(0, nk // 2)
    def _(i):
        for cp in w_copies(i):
            cp.start()
        for t in range(2):
            k_copy(i * 2 + t).wait()
            v_copy(i * 2 + t).wait()
        seqs = [(i * 2 + t, j, (i * 2 + t) * kb + j) for t in range(2) for j in range(kb)]
        for n, (ch, j, b_i) in enumerate(seqs):
            q = qs[of(b_i), :].astype(BF16)
            s = lax.dot_general(q, k_v[ch, j], (((1,), (1,)), ((), ())), preferred_element_type=F32) * 128 ** -0.5
            sc[n] = jnp.where(pos < lens_ref[b_i], s, -jnp.inf)
        ps = []
        for n in range(len(seqs)):
            s = sc[n]
            p = jnp.exp(s - jnp.max(s, axis=-1, keepdims=True))
            ps.append((p * (1.0 / jnp.sum(p, axis=-1, keepdims=True))).astype(BF16))
        for p, (ch, j, b_i) in zip(ps, seqs):
            qs[of(b_i), :] = jnp.dot(p, v_v[ch, j], preferred_element_type=F32)

    ahead = nk // 2
    while 2 * (ahead + 1) + nq <= RING:
        for cp in w_copies(ahead):
            cp.start()
        ahead += 1

    for hh in range(nh):
        ob[:, hh * 128:(hh + 1) * 128] = qs[pl.ds(hh, b, stride=nh), :].astype(BF16)

    no = d // CH

    def source(o, core):
        oz, oy, ox = _offset((z, y, x), o)
        return ((oz * 2 + oy) * 2 + ox) * 2 + core

    def send(o, i):
        via = {3: (1, 2), 6: (2, 4), 5: (4, 1), 7: ((3, 4), (6, 1), (5, 2))[i % 3]}
        held, to = via.get(o, (0, o))
        src = ha.at[source(held, c), :, cols(i)] if held else h_ref.at[:, cols(i)]
        dev = _dev(*_offset((z, y, x), to), c) if o else _dev(z, y, x, 1 - c)
        return pltpu.make_async_remote_copy(src, ha.at[source(held, c), :, cols(i)], us_send.at[o, i],
                                            us_recv.at[o, i], device_id=dev, device_id_type=MESH)

    def forward(o, i):
        at = ha.at[source(o, c), :, cols(i)]
        return pltpu.make_async_remote_copy(at, at, uf_send.at[o, i], uf_recv.at[o, i],
                                            device_id=_dev(z, y, x, 1 - c), device_id_type=MESH)

    def store(o, core):
        src = source(o, core)
        return pltpu.make_async_copy(ua.at[src], uall_hbm.at[src], out_sem.at[2 * o + (0 if core is c else 1)])

    def arrived(level, i):
        for o in ((1, 2, 4), (3, 6, 5), (7,))[level]:
            send(o, i).wait_recv()
            if level == 0:
                send({1: 3, 2: 6, 4: 5}[o], i).start()
            if level == 1 and o == (3, 6, 5)[i % 3]:
                send(7, i).start()
            forward(o, i).start()

    order = (1, 2, 4, 3, 6, 5, 7)
    for i in range(no):
        acc = x_ref[:, cols(i)].astype(F32)
        attn = jnp.zeros((b, CH), F32)
        for t in range(2):
            o_copy(i * 2 + t).wait()
            attn += jnp.dot(ob[:, t * d:(t + 1) * d], ring[lax.rem(nq + i * 2 + t, RING)], preferred_element_type=F32)
        h_ref[:, cols(i)] = (acc + attn).astype(BF16)
        for cp in w_copies(ahead + i) if ahead + i < nw else ():
            cp.start()
        for o in (1, 2, 4, 0):
            send(o, i).start()

    ahead = min(ahead + no, nw)
    ln2 = _row(ln2_ref)
    us[...] = _rms(h_ref[...].astype(F32), ln2)

    def shared(i):
        c1, c3 = w_copies(i)
        c1.wait()
        c3.wait()
        s = lax.rem(2 * nq + 2 * i, RING)
        z1 = jnp.dot(us[...], ring[s], preferred_element_type=F32)
        z3 = jnp.dot(us[...], ring[s + 1], preferred_element_type=F32)
        g_ref[:, cols(i)] = _silu_mul(z1, z3)

    ua[me] = us[...]
    shared(0)
    arrived(0, 0)
    arrived(0, 1)

    n = 0
    while ahead < nw:
        for cp in w_copies(ahead):
            cp.start()
        ahead += 1
        n += 1
        if ahead < nw:
            shared(n)

    for o in range(1, 16):
        m_send(o).wait_recv()
    base = ((lax.axis_index("ey") * 8 + lax.axis_index("ex")) * EDEV).astype(F32)
    turned = ma[...].reshape(128, 128).T
    lane = lax.broadcasted_iota(jnp.int32, (b, 128), 1).astype(F32) + base
    nblk = ma.shape[0]
    for i in range(nblk):
        hb = jnp.zeros((b, 128), F32)
        gb = jnp.zeros((b, 128), F32)
        for j in range(TOP):
            at = i * 2 * TOP + j
            same = turned[0:b, at:at + 1] == lane
            hb += jnp.where(same, 1.0, 0.0)
            gb += jnp.where(same, turned[0:b, at + TOP:at + TOP + 1], 0.0)
        hit[i * b:(i + 1) * b, :] = hb
        gsel_ref[i * b:(i + 1) * b, :] = gb
    r0 = lax.broadcasted_iota(jnp.int32, (GROUP, GROUP), 0)
    r1 = lax.broadcasted_iota(jnp.int32, (GROUP, GROUP), 1)
    before = jnp.where(r1 < r0, 1.0, 0.0)
    before_blk = jnp.where(r1 // b == r0 // b, before, 0.0).astype(BF16)
    before = before.astype(BF16)
    for g in range(nblk * b // GROUP):
        sl = slice(g * GROUP, (g + 1) * GROUP)
        rank = jnp.dot(before_blk, hit[sl, :].astype(BF16), preferred_element_type=F32)
        keep = jnp.where(rank < cap, hit[sl, :], 0.0)
        at = jnp.dot(before, keep.astype(BF16), preferred_element_type=F32)
        key = jnp.where(keep > 0.0, at, -1.0)
        key_ref[sl, :] = key
        krow_ref[:, sl] = key.T[0:8]
        cnt_ref[g:g + 1, :] = jnp.sum(keep, axis=0, keepdims=True).astype(jnp.int32)

    def normalise(o, core):
        src = source(o, core)
        ua[src] = _rms(ha[src].astype(F32), ln2)

    for i in range(n if n else 1, nw):
        shared(i)
        for step in {1: ((0, 2), (1, 0)), 2: ((0, 3), (1, 1)), 3: ((1, 2), (2, 0)), 4: ((1, 3), (2, 1)),
                     5: ((2, 2), (2, 3))}.get(i, ()):
            arrived(*step)
        if i == nw - 3:
            for o in order:
                normalise(o, c)
            for o in range(8):
                store(o, c).start()
        if i == nw - 2:
            for t in range(no):
                send(0, t).wait_recv()
            for o in order:
                for t in range(no):
                    forward(o, t).wait_recv()
            for o in range(8):
                normalise(o, 1 - c)
            for o in range(8):
                store(o, 1 - c).start()

    for o in range(8):
        for t in range(no):
            send(o, t).wait_send()
            if o:
                forward(o, t).wait_send()
        store(o, c).wait()
        store(o, 1 - c).wait()
    for o in range(1, 16):
        m_send(o).wait_send()


def _row(ref):
    return jnp.concatenate([ref[i:i + 1, :] for i in range(ref.shape[0])], axis=1)


def _front(x, k, v, lens, idx, gates, ln1, ln2, wq, wo, ws1, ws3):
    b, d = x.shape
    nqk, fs = wq.shape[1], ws1.shape[1] - LATE * CH
    rows = k.shape[1] * k.shape[2]
    nk = 8
    ndev = 16
    k = k.reshape(nk, b // nk, rows, 128)
    v = v.reshape(nk, b // nk, rows, 128)
    nh = nqk // 128
    t = ndev * b
    return pl.pallas_call(
        functools.partial(_front_kernel, b - b // 8),
        out_shape=[jax.ShapeDtypeStruct((b, d), BF16)] * 2 + [jax.ShapeDtypeStruct((ndev, b, d), BF16),
                   jax.ShapeDtypeStruct((b, fs), BF16), jax.ShapeDtypeStruct((t, 128), F32),
                   jax.ShapeDtypeStruct((t, 128), F32), jax.ShapeDtypeStruct((8, t), F32),
                   jax.ShapeDtypeStruct((t // GROUP, 128), jnp.int32)],
        in_specs=[VMEM] * 5 + [SMEM] + [HBM] * 6,
        out_specs=[VMEM, VMEM, HBM] + [VMEM] * 5,
        scratch_shapes=[
            pltpu.VMEM((RING, d, CH), BF16),
            pltpu.VMEM((nk, b // nk, rows, 128), BF16),
            pltpu.VMEM((nk, b // nk, rows, 128), BF16),
            pltpu.VMEM((b * nh, 128), F32),
            pltpu.VMEM((b // 4, nh, rows), F32),
            pltpu.VMEM((b, nqk), BF16),
            pltpu.VMEM((ndev, b, d), BF16),
            pltpu.VMEM((ndev, b, d), BF16),
            pltpu.VMEM((2 * TOP, 128), F32),
            pltpu.VMEM((ndev, 2 * TOP, 128), F32),
            pltpu.VMEM((t, 128), F32),
            DMA((RING,)), DMA((nk,)), DMA((nk,)), DMA((16,)),
            DMA((8, d // CH)), DMA((8, d // CH)), DMA((8, d // CH)), DMA((8, d // CH)), DMA((16,)), DMA((16,)),
        ],
        compiler_params=pltpu.CompilerParams(vmem_limit_bytes=63 * 2 ** 20, collective_id=0, has_side_effects=True),
        name="front",
    )(x, ln1.reshape(d // 128, 128), ln2.reshape(d // 128, 128), idx.T, gates.T, lens, wq, k, v, wo, ws1, ws3)


SMALL = 32


def _expert_kernel(big, u_hbm, key_hbm, gsel_hbm, krow, cnt, w1_hbm, w3_hbm, w2_hbm, p_ref,
                   u_v, xs, zs, w1_v, w3_v, w2_v, mid, key_ref, gsel_ref, order, u_sem, k_sem, w_sem):
    t, d = u_v.shape
    ng = t // GROUP
    u_copy = pltpu.make_async_copy(u_hbm, u_v, u_sem)
    u_copy.start()
    for e in range(EDEV):
        n = cnt[0, e] + cnt[1, e]
        rank = 0
        for f in range(EDEV):
            if f != e:
                m = cnt[0, f] + cnt[1, f]
                rank += ((m >= n) if f < e else (m > n)).astype(jnp.int32)
        order[rank] = e

    def copy(i, hbm, vm, k):
        s = lax.rem(i, 2)
        return pltpu.make_async_copy(hbm.at[order[i]], vm.at[s], w_sem.at[s, k])

    def w1_copy(i):
        return copy(i, w1_hbm, w1_v, 0)

    def w3_copy(i):
        return copy(i, w3_hbm, w3_v, 1)

    def w2_copy(i):
        return copy(i, w2_hbm, w2_v, 2)

    for i in range(2):
        w1_copy(i).start()
        w3_copy(i).start()
        w2_copy(i).start()
        if i == 0:
            k_copies = (pltpu.make_async_copy(key_hbm, key_ref, k_sem.at[0]),
                        pltpu.make_async_copy(gsel_hbm, gsel_ref, k_sem.at[1]))
            for cp in k_copies:
                cp.start()
    p_ref[...] = jnp.zeros_like(p_ref)
    u_copy.wait()
    lane = lax.broadcasted_iota(jnp.int32, (GROUP, 128), 1)

    def tokens(g):
        return pl.ds(g * GROUP if isinstance(g, int) else pl.multiple_of(g * GROUP, GROUP), GROUP)

    def pick(e, g, n):
        r = lax.broadcasted_iota(jnp.int32, (n, GROUP), 0).astype(F32)
        sel = jnp.where(krow[pl.ds(e, 1), tokens(g)] == r, 1.0, 0.0).astype(BF16)
        return jnp.dot(sel, u_v[tokens(g), :], preferred_element_type=F32).astype(BF16)

    def put(e, g, n, out):
        tl = tokens(g)
        r = lax.broadcasted_iota(jnp.int32, (GROUP, 128), 1).astype(F32)
        key = jnp.sum(jnp.where(lane == e, key_ref[tl, :], 0.0), axis=1, keepdims=True)
        sel = jnp.concatenate([jnp.where(key == r + 128.0 * q, 1.0, 0.0) for q in range(-(-n // 128))], axis=1)
        sel = sel[:, :n].astype(BF16)
        gt = jnp.sum(jnp.where(lane == e, gsel_ref[tl, :], 0.0), axis=1, keepdims=True)
        for q in range(d // 256):
            cs = slice(q * 256, (q + 1) * 256)
            back = jnp.dot(sel, out[:, cs], preferred_element_type=F32)
            p_ref[tl, cs] += back * gt

    def slots(g):
        return pl.ds(pl.multiple_of(g * big, 16), big)

    def down(g, s):
        return jnp.dot(g, w2_v[s], preferred_element_type=F32).astype(BF16)

    @pl.loop(0, EDEV)
    def _(i):
        e, s = order[i], lax.rem(i, 2)
        most = jnp.maximum(cnt[0, e], cnt[1, e])
        few = jnp.logical_and(most > 0, most <= SMALL)
        many = most > SMALL
        both = slice(0, ng * SMALL)

        @pl.when(few)
        def _():
            for g in range(ng):
                xs[g * SMALL:(g + 1) * SMALL, :] = pick(e, g, SMALL)

        @pl.when(many)
        def _():
            @pl.loop(0, ng)
            def _(g):
                xs[slots(g), :] = pick(e, g, big)

        w1_copy(i).wait()

        @pl.when(few)
        def _():
            zs[both, :] = jnp.dot(xs[both, :], w1_v[s], preferred_element_type=F32)

        @pl.when(many)
        def _():
            @pl.loop(0, ng)
            def _(g):
                zs[slots(g), :] = jnp.dot(xs[slots(g), :], w1_v[s], preferred_element_type=F32)

        @pl.when(i + 2 < EDEV)
        def _():
            w1_copy(i + 2).start()

        w3_copy(i).wait()

        @pl.when(few)
        def _():
            mid[both, :] = _silu_mul(zs[both, :], jnp.dot(xs[both, :], w3_v[s], preferred_element_type=F32))

        @pl.when(many)
        def _():
            @pl.loop(0, ng)
            def _(g):
                mid[slots(g), :] = _silu_mul(
                    zs[slots(g), :], jnp.dot(xs[slots(g), :], w3_v[s], preferred_element_type=F32))

        @pl.when(i + 2 < EDEV)
        def _():
            w3_copy(i + 2).start()

        w2_copy(i).wait()

        @pl.when(i == 0)
        def _():
            for cp in k_copies:
                cp.wait()

        @pl.when(few)
        def _():
            out = down(mid[both, :], s)
            for g in range(ng):
                put(e, g, SMALL, out[g * SMALL:(g + 1) * SMALL])

        @pl.when(many)
        def _():
            @pl.loop(0, ng)
            def _(g):
                put(e, g, big, down(mid[slots(g), :], s))

        @pl.when(i + 2 < EDEV)
        def _():
            w2_copy(i + 2).start()


def _experts(u, key, gsel, krow, cnt, w1, w3, w2, blk):
    t, d = u.shape
    f = w1.shape[2]
    big = (blk - blk // 8) * (GROUP // blk)
    slots = big * (t // GROUP)
    return pl.pallas_call(
        functools.partial(_expert_kernel, big),
        out_shape=jax.ShapeDtypeStruct((t, d), F32),
        in_specs=[HBM, HBM, HBM, VMEM, SMEM, HBM, HBM, HBM],
        out_specs=VMEM,
        scratch_shapes=[
            pltpu.VMEM((t, d), BF16),
            pltpu.VMEM((slots, d), BF16),
            pltpu.VMEM((slots, f), F32),
            pltpu.VMEM((2, d, f), BF16),
            pltpu.VMEM((2, d, f), BF16),
            pltpu.VMEM((2, f, d), BF16),
            pltpu.VMEM((slots, f), BF16),
            pltpu.VMEM((t, 128), F32),
            pltpu.VMEM((t, 128), F32),
            pltpu.SMEM((EDEV,), jnp.int32),
            DMA(()), DMA((2,)), DMA((2, 3)),
        ],
        compiler_params=pltpu.CompilerParams(vmem_limit_bytes=55 * 2 ** 20),
        name="experts",
    )(u, key, gsel, krow, cnt, w1, w3, w2)


COLS = ((0, 640), (640, 640), (1280, 768))
PARTS, ROWS = 4, 8
NS = 3 * PARTS


def _combine_kernel(p_hbm, g_ref, h_ref, u_ref, ws1_hbm, ws3_hbm, w_hbm, y_ref,
                    acc, r0, r1, r2, r3, w_v, a_v, b_v, late, sh, w_sem, a_sem, b_sem, p_sem,
                    s0, q0, s1, q1, s2, q2, s3, q3):
    z, y, x, c = _place()
    nw, _, wn = w_v.shape

    def w_copy(i):
        return pltpu.make_async_copy(w_hbm.at[:, pl.ds(i * wn, wn)], w_v.at[i], w_sem.at[i])

    streams = [(p, half) for half in range(PARTS) for p in range(3)]
    place = {0: x, 1: y, 2: z}

    def cols(p):
        return pl.ds(COLS[p][0], COLS[p][1])

    def rows(half):
        return pl.ds(half * ROWS, ROWS)

    early = g_ref.shape[1]

    def a_copy(i):
        return pltpu.make_async_copy(ws1_hbm.at[:, pl.ds(early + i * CH, CH)], a_v.at[i], a_sem.at[i])

    def b_copy(i):
        return pltpu.make_async_copy(ws3_hbm.at[:, pl.ds(early + i * CH, CH)], b_v.at[i], b_sem.at[i])

    def load(k):
        p, half = streams[k]
        return pltpu.make_async_copy(p_hbm.at[:, :, :, c, rows(half), cols(p)], acc.at[:, :, :, rows(half), cols(p)],
                                     p_sem.at[k])

    def swap(k):
        p, half = streams[k]
        return pltpu.make_async_remote_copy(
            p_hbm.at[:, :, :, 1 - c, rows(half), cols(p)], r0.at[:, :, :, rows(half), cols(p)], s0.at[k], q0.at[k],
            device_id=_dev(z, y, x, 1 - c), device_id_type=MESH)

    def region(ref, p, half, step, mine):
        ix = [pl.ds(0, 2)] * 3
        for s in range(step):
            dim = (p + s) % 3
            v = place[dim]
            ix[2 - dim] = v if (s < step - 1 or mine) else 1 - v
        return ref.at[ix[0], ix[1], ix[2], rows(half), cols(p)]

    def landing(p, half, step):
        ref = (r1, r2, r3)[step - 1]
        if step == 1:
            return ref.at[:, :, rows(half), cols(p)]
        if step == 2:
            return ref.at[:, rows(half), cols(p)]
        return ref.at[rows(half), cols(p)]

    def hop(k, step):
        p, half = streams[k]
        dim = (p + step - 1) % 3
        o = [z, y, x]
        o[2 - dim] = 1 - o[2 - dim]
        send, recv = ((s1, q1), (s2, q2), (s3, q3))[step - 1]
        return pltpu.make_async_remote_copy(
            region(acc, p, half, step, False), landing(p, half, step), send.at[k], recv.at[k],
            device_id=_dev(*o, c), device_id_type=MESH)

    for k in range(NS):
        load(k).start()
    for i in range(LATE):
        a_copy(i).start()
        b_copy(i).start()
    barrier = pltpu.get_barrier_semaphore()
    pl.semaphore_signal(barrier, inc=1, device_id=_dev(z, y, x, 1 - c), device_id_type=MESH)
    for d in (1, 2, 4):
        pl.semaphore_signal(barrier, inc=1, device_id=_dev(*_offset((z, y, x), d), c), device_id_type=MESH)
    pl.semaphore_wait(barrier, 4)
    for k in range(NS):
        swap(k).start()
    for i in range(nw):
        w_copy(i).start()

    def shared(i):
        w_copy(i).wait()
        cs = slice(i * wn, (i + 1) * wn)
        s = jnp.dot(g_ref[...], w_v[i, 0:early], preferred_element_type=F32)
        s += jnp.dot(late[...], w_v[i, early:], preferred_element_type=F32)
        sh[:, cs] = s + h_ref[:, cs].astype(F32)

    def up(i):
        a_copy(i).wait()
        b_copy(i).wait()
        late[:, i * CH:(i + 1) * CH] = _silu_mul(jnp.dot(u_ref[...], a_v[i], preferred_element_type=F32),
                                                 jnp.dot(u_ref[...], b_v[i], preferred_element_type=F32))

    for k in range(NS):
        p, half = streams[k]
        load(k).wait()
        swap(k).wait_recv()
        rs, cs = slice(half * ROWS, half * ROWS + ROWS), slice(COLS[p][0], COLS[p][0] + COLS[p][1])
        acc[:, :, :, rs, cs] += r0[:, :, :, rs, cs]
        hop(k, 1).start()
    for i in range(LATE):
        up(i)

    def add(k, step):
        p, half = streams[k]
        hop(k, step).wait_recv()
        v = region(acc, p, half, step, True)
        if step < 3:
            v[...] += landing(p, half, step)[...]
            hop(k, step + 1).start()
        else:
            tot = v[...] + landing(p, half, 3)[...]
            rs, cs = slice(half * ROWS, half * ROWS + ROWS), slice(COLS[p][0], COLS[p][0] + COLS[p][1])
            y_ref[rs, cs] = (sh[rs, cs] + tot).astype(BF16)

    for k in range(NS):
        add(k, 1)
        if k % 3 == 2:
            shared(k // 3)
        if k >= 6:
            add(k - 6, 2)
    for k in range(6, NS):
        add(k, 2)
    for k in range(NS):
        add(k, 3)
    for k in range(NS):
        swap(k).wait_send()
        for step in (1, 2, 3):
            hop(k, step).wait_send()


def _combine(part, g, h, u, ws1, ws3, ws2):
    b, d = h.shape
    fs = ws2.shape[0]
    nw = 4
    part = part.reshape(2, 2, 2, 2, b, d)
    return pl.pallas_call(
        _combine_kernel,
        out_shape=jax.ShapeDtypeStruct((b, d), BF16),
        in_specs=[HBM, VMEM, VMEM, VMEM, HBM, HBM, HBM],
        out_specs=VMEM,
        scratch_shapes=[
            pltpu.VMEM((2, 2, 2, b, d), F32),
            pltpu.VMEM((2, 2, 2, b, d), F32),
            pltpu.VMEM((2, 2, b, d), F32),
            pltpu.VMEM((2, b, d), F32),
            pltpu.VMEM((b, d), F32),
            pltpu.VMEM((nw, fs, d // nw), BF16),
            pltpu.VMEM((LATE, d, CH), BF16),
            pltpu.VMEM((LATE, d, CH), BF16),
            pltpu.VMEM((b, LATE * CH), BF16),
            pltpu.VMEM((b, d), F32),
            DMA((nw,)), DMA((LATE,)), DMA((LATE,)), DMA((NS,)),
            DMA((NS,)), DMA((NS,)), DMA((NS,)), DMA((NS,)), DMA((NS,)), DMA((NS,)), DMA((NS,)), DMA((NS,)),
        ],
        compiler_params=pltpu.CompilerParams(vmem_limit_bytes=50 * 2 ** 20, collective_id=1, has_side_effects=True),
        name="combine",
    )(part, g, h, u, ws1, ws3, ws2)


def solution(mesh):
    def body(x, kv_k, kv_v, lens, idx, gates, ln1, wq, wo, ln2, ws1, ws3, ws2, w1, w3, w2):
        b, d = x.shape
        h, u, uall, g, key, gsel, krow, cnt = _front(x, kv_k, kv_v, lens, idx, gates, ln1, ln2, wq, wo, ws1, ws3)
        part = _experts(uall.reshape(16 * b, d), key, gsel, krow, cnt, w1, w3, w2, b)
        return _combine(part, g, h, u, ws1, ws3, ws2)

    rows = P(GRP)
    rep = P()
    return jax.shard_map(
        body, mesh=mesh,
        in_specs=(rows, rows, rows, rows, rows, rows, rep, rep, rep, rep, rep, rep, rep, rows, rows, rows),
        out_specs=rows, check_vma=False)
```

```python
import functools

import jax
import jax.numpy as jnp
from jax import lax
from jax.experimental import pallas as pl
from jax.experimental.pallas import tpu as pltpu
from jax.sharding import PartitionSpec as P

EPS = 1e-6
GRP = ("ey", "ex")
F32 = jnp.float32
BF16 = jnp.bfloat16
MESH = pl.DeviceIdType.MESH
VMEM = pl.BlockSpec(memory_space=pltpu.VMEM)
SMEM = pl.BlockSpec(memory_space=pltpu.SMEM)
HBM = pl.BlockSpec(memory_space=pltpu.HBM)
DMA = pltpu.SemaphoreType.DMA
TOP = 4
EDEV = 4


def _rms(v32, w):
    r = lax.rsqrt(jnp.mean(v32 * v32, axis=-1, keepdims=True) + EPS)
    return (v32 * r * w.astype(F32)).astype(BF16)


def _silu_mul(z1, z3):
    return (jax.nn.silu(z1) * z3).astype(BF16)


def _place():
    z = lax.axis_index("ey")
    ex = lax.axis_index("ex")
    return z, ex // 4, (ex // 2) % 2, ex % 2


def _dev(z, y, x, c):
    return (z, y * 4 + x * 2 + c)


def _flip(v, f):
    return 1 - v if f else v


def _offset(place, d):
    z, y, x = place
    return _flip(z, d // 4), _flip(y, (d // 2) % 2), _flip(x, d % 2)


CH = 512
RING = 16
LATE = 3
GROUP = 256


def _front_kernel(cap, x_ref, ln1_ref, ln2_ref, idx_ref, gate_ref, lens_ref, wq_hbm, k_hbm, v_hbm, wo_hbm, ws1_hbm,
                  ws3_hbm, h_ref, us, uall_hbm, g_ref, key_ref, gsel_ref, krow_ref, cnt_ref,
                  ring, k_v, v_v, qs, sc, ob, ha, ua, ms, ma, hit,
                  r_sem, k_sem, v_sem, out_sem, us_send, us_recv, uf_send, uf_recv, ms_send, ms_recv):
    b, d = x_ref.shape
    nqk = wq_hbm.shape[1]
    nh = nqk // 128
    nq = nqk // CH
    nk, kb, rows = k_v.shape[:3]
    nw = ws1_hbm.shape[1] // CH - LATE
    z, y, x, c = _place()
    me = ((z * 2 + y) * 2 + x) * 2 + c

    def cols(i):
        return pl.ds(i * CH if isinstance(i, int) else pl.multiple_of(i * CH, CH), CH)

    def chunk(src, n):
        s = lax.rem(n, RING)
        return pltpu.make_async_copy(src, ring.at[s], r_sem.at[s])

    def q_copy(i):
        return chunk(wq_hbm.at[:, cols(i)], i)

    def o_copy(i):
        return chunk(wo_hbm.at[pl.ds(pl.multiple_of((i % 2) * d, d), d), cols(i // 2)], nq + i)

    def w_copies(i):
        return chunk(ws1_hbm.at[:, cols(i)], 2 * nq + 2 * i), chunk(ws3_hbm.at[:, cols(i)], 2 * nq + 2 * i + 1)

    def k_copy(i):
        return pltpu.make_async_copy(k_hbm.at[i], k_v.at[i], k_sem.at[i])

    def v_copy(i):
        return pltpu.make_async_copy(v_hbm.at[i], v_v.at[i], v_sem.at[i])

    for i in range(nq):
        q_copy(i).start()
    barrier = pltpu.get_barrier_semaphore()
    peers = [_dev(*_offset((z, y, x), o % 8), _flip(c, o // 8)) for o in range(1, 16)]
    for dev in peers:
        pl.semaphore_signal(barrier, inc=1, device_id=dev, device_id_type=MESH)
    ms[...] = jnp.zeros_like(ms)
    ms[0:TOP, 0:b] = idx_ref[...].astype(F32)
    ms[TOP:2 * TOP, 0:b] = gate_ref[...]
    a = _rms(x_ref[...].astype(F32), _row(ln1_ref))

    @pl.loop(0, nq)
    def _(i):
        k_copy(i).start()
        v_copy(i).start()
        q_copy(i).wait()
        q = jnp.dot(a, ring[i], preferred_element_type=F32).astype(BF16).astype(F32)
        for j in range(CH // 128):
            qs[pl.ds(i * (CH // 128) + j, b, stride=nh), :] = q[:, j * 128:(j + 1) * 128]

    for i in range(2 * d // CH):
        o_copy(i).start()
    pl.semaphore_wait(barrier, 15)

    def m_send(o):
        return pltpu.make_async_remote_copy(ms, ma.at[me], ms_send.at[o], ms_recv.at[o], device_id=peers[o - 1],
                                            device_id_type=MESH)

    for o in range(1, 16):
        m_send(o).start()
    ma[me] = ms[...]

    kvh = 4
    row = lax.broadcasted_iota(jnp.int32, (nh, rows), 1)
    head = lax.broadcasted_iota(jnp.int32, (nh, rows), 0)
    pos = jnp.where(row % kvh == head // (nh // kvh), row // kvh, rows)

    def of(i):
        return pl.ds(pl.multiple_of(i * nh, nh), nh)

    @pl.loop(0, nk // 2)
    def _(i):
        for cp in w_copies(i):
            cp.start()
        for t in range(2):
            k_copy(i * 2 + t).wait()
            v_copy(i * 2 + t).wait()
        seqs = [(i * 2 + t, j, (i * 2 + t) * kb + j) for t in range(2) for j in range(kb)]
        for n, (ch, j, b_i) in enumerate(seqs):
            q = qs[of(b_i), :].astype(BF16)
            s = lax.dot_general(q, k_v[ch, j], (((1,), (1,)), ((), ())), preferred_element_type=F32) * 128 ** -0.5
            sc[n] = jnp.where(pos < lens_ref[b_i], s, -jnp.inf)
        ps = []
        for n in range(len(seqs)):
            s = sc[n]
            p = jnp.exp(s - jnp.max(s, axis=-1, keepdims=True))
            ps.append((p * (1.0 / jnp.sum(p, axis=-1, keepdims=True))).astype(BF16))
        for p, (ch, j, b_i) in zip(ps, seqs):
            qs[of(b_i), :] = jnp.dot(p, v_v[ch, j], preferred_element_type=F32)

    ahead = nk // 2
    while 2 * (ahead + 1) + nq <= RING:
        for cp in w_copies(ahead):
            cp.start()
        ahead += 1

    for hh in range(nh):
        ob[:, hh * 128:(hh + 1) * 128] = qs[pl.ds(hh, b, stride=nh), :].astype(BF16)

    no = d // CH

    def source(o, core):
        oz, oy, ox = _offset((z, y, x), o)
        return ((oz * 2 + oy) * 2 + ox) * 2 + core

    def send(o, i):
        via = {3: (1, 2), 6: (2, 4), 5: (4, 1), 7: ((3, 4), (6, 1), (5, 2))[i % 3]}
        held, to = via.get(o, (0, o))
        src = ha.at[source(held, c), :, cols(i)] if held else h_ref.at[:, cols(i)]
        dev = _dev(*_offset((z, y, x), to), c) if o else _dev(z, y, x, 1 - c)
        return pltpu.make_async_remote_copy(src, ha.at[source(held, c), :, cols(i)], us_send.at[o, i],
                                            us_recv.at[o, i], device_id=dev, device_id_type=MESH)

    def forward(o, i):
        at = ha.at[source(o, c), :, cols(i)]
        return pltpu.make_async_remote_copy(at, at, uf_send.at[o, i], uf_recv.at[o, i],
                                            device_id=_dev(z, y, x, 1 - c), device_id_type=MESH)

    def store(o, core):
        src = source(o, core)
        return pltpu.make_async_copy(ua.at[src], uall_hbm.at[src], out_sem.at[2 * o + (0 if core is c else 1)])

    def arrived(level, i):
        for o in ((1, 2, 4), (3, 6, 5), (7,))[level]:
            send(o, i).wait_recv()
            if level == 0:
                send({1: 3, 2: 6, 4: 5}[o], i).start()
            if level == 1 and o == (3, 6, 5)[i % 3]:
                send(7, i).start()
            forward(o, i).start()

    order = (1, 2, 4, 3, 6, 5, 7)
    for i in range(no):
        acc = x_ref[:, cols(i)].astype(F32)
        attn = jnp.zeros((b, CH), F32)
        for t in range(2):
            o_copy(i * 2 + t).wait()
            attn += jnp.dot(ob[:, t * d:(t + 1) * d], ring[lax.rem(nq + i * 2 + t, RING)], preferred_element_type=F32)
        h_ref[:, cols(i)] = (acc + attn).astype(BF16)
        for cp in w_copies(ahead + i) if ahead + i < nw else ():
            cp.start()
        for o in (1, 2, 4, 0):
            send(o, i).start()

    ahead = min(ahead + no, nw)
    ln2 = _row(ln2_ref)
    us[...] = _rms(h_ref[...].astype(F32), ln2)

    def shared(i):
        c1, c3 = w_copies(i)
        c1.wait()
        c3.wait()
        s = lax.rem(2 * nq + 2 * i, RING)
        z1 = jnp.dot(us[...], ring[s], preferred_element_type=F32)
        z3 = jnp.dot(us[...], ring[s + 1], preferred_element_type=F32)
        g_ref[:, cols(i)] = _silu_mul(z1, z3)

    ua[me] = us[...]
    shared(0)
    arrived(0, 0)
    arrived(0, 1)

    n = 0
    while ahead < nw:
        for cp in w_copies(ahead):
            cp.start()
        ahead += 1
        n += 1
        if ahead < nw:
            shared(n)

    for o in range(1, 16):
        m_send(o).wait_recv()
    base = ((lax.axis_index("ey") * 8 + lax.axis_index("ex")) * EDEV).astype(F32)
    turned = ma[...].reshape(128, 128).T
    lane = lax.broadcasted_iota(jnp.int32, (b, 128), 1).astype(F32) + base
    nblk = ma.shape[0]
    for i in range(nblk):
        hb = jnp.zeros((b, 128), F32)
        gb = jnp.zeros((b, 128), F32)
        for j in range(TOP):
            at = i * 2 * TOP + j
            same = turned[0:b, at:at + 1] == lane
            hb += jnp.where(same, 1.0, 0.0)
            gb += jnp.where(same, turned[0:b, at + TOP:at + TOP + 1], 0.0)
        hit[i * b:(i + 1) * b, :] = hb
        gsel_ref[i * b:(i + 1) * b, :] = gb
    r0 = lax.broadcasted_iota(jnp.int32, (GROUP, GROUP), 0)
    r1 = lax.broadcasted_iota(jnp.int32, (GROUP, GROUP), 1)
    before = jnp.where(r1 < r0, 1.0, 0.0)
    before_blk = jnp.where(r1 // b == r0 // b, before, 0.0).astype(BF16)
    before = before.astype(BF16)
    for g in range(nblk * b // GROUP):
        sl = slice(g * GROUP, (g + 1) * GROUP)
        rank = jnp.dot(before_blk, hit[sl, :].astype(BF16), preferred_element_type=F32)
        keep = jnp.where(rank < cap, hit[sl, :], 0.0)
        at = jnp.dot(before, keep.astype(BF16), preferred_element_type=F32)
        key = jnp.where(keep > 0.0, at, -1.0)
        key_ref[sl, :] = key
        krow_ref[:, sl] = key.T[0:8]
        cnt_ref[g:g + 1, :] = jnp.sum(keep, axis=0, keepdims=True).astype(jnp.int32)

    def normalise(o, core):
        src = source(o, core)
        ua[src] = _rms(ha[src].astype(F32), ln2)

    for i in range(n if n else 1, nw):
        shared(i)
        for step in {1: ((0, 2), (1, 0)), 2: ((0, 3), (1, 1)), 3: ((1, 2), (2, 0)), 4: ((1, 3), (2, 1)),
                     5: ((2, 2), (2, 3))}.get(i, ()):
            arrived(*step)
        if i == nw - 3:
            for o in order:
                normalise(o, c)
            for o in range(8):
                store(o, c).start()
        if i == nw - 2:
            for t in range(no):
                send(0, t).wait_recv()
            for o in order:
                for t in range(no):
                    forward(o, t).wait_recv()
            for o in range(8):
                normalise(o, 1 - c)
            for o in range(8):
                store(o, 1 - c).start()

    for o in range(8):
        for t in range(no):
            send(o, t).wait_send()
            if o:
                forward(o, t).wait_send()
        store(o, c).wait()
        store(o, 1 - c).wait()
    for o in range(1, 16):
        m_send(o).wait_send()


def _row(ref):
    return jnp.concatenate([ref[i:i + 1, :] for i in range(ref.shape[0])], axis=1)


def _front(x, k, v, lens, idx, gates, ln1, ln2, wq, wo, ws1, ws3):
    b, d = x.shape
    nqk, fs = wq.shape[1], ws1.shape[1] - LATE * CH
    rows = k.shape[1] * k.shape[2]
    nk = 8
    ndev = 16
    k = k.reshape(nk, b // nk, rows, 128)
    v = v.reshape(nk, b // nk, rows, 128)
    nh = nqk // 128
    t = ndev * b
    return pl.pallas_call(
        functools.partial(_front_kernel, b - b // 8),
        out_shape=[jax.ShapeDtypeStruct((b, d), BF16)] * 2 + [jax.ShapeDtypeStruct((ndev, b, d), BF16),
                   jax.ShapeDtypeStruct((b, fs), BF16), jax.ShapeDtypeStruct((t, 128), F32),
                   jax.ShapeDtypeStruct((t, 128), F32), jax.ShapeDtypeStruct((8, t), F32),
                   jax.ShapeDtypeStruct((t // GROUP, 128), jnp.int32)],
        in_specs=[VMEM] * 5 + [SMEM] + [HBM] * 6,
        out_specs=[VMEM, VMEM, HBM] + [VMEM] * 5,
        scratch_shapes=[
            pltpu.VMEM((RING, d, CH), BF16),
            pltpu.VMEM((nk, b // nk, rows, 128), BF16),
            pltpu.VMEM((nk, b // nk, rows, 128), BF16),
            pltpu.VMEM((b * nh, 128), F32),
            pltpu.VMEM((b // 4, nh, rows), F32),
            pltpu.VMEM((b, nqk), BF16),
            pltpu.VMEM((ndev, b, d), BF16),
            pltpu.VMEM((ndev, b, d), BF16),
            pltpu.VMEM((2 * TOP, 128), F32),
            pltpu.VMEM((ndev, 2 * TOP, 128), F32),
            pltpu.VMEM((t, 128), F32),
            DMA((RING,)), DMA((nk,)), DMA((nk,)), DMA((16,)),
            DMA((8, d // CH)), DMA((8, d // CH)), DMA((8, d // CH)), DMA((8, d // CH)), DMA((16,)), DMA((16,)),
        ],
        compiler_params=pltpu.CompilerParams(vmem_limit_bytes=63 * 2 ** 20, collective_id=0, has_side_effects=True),
        name="front",
    )(x, ln1.reshape(d // 128, 128), ln2.reshape(d // 128, 128), idx.T, gates.T, lens, wq, k, v, wo, ws1, ws3)


SMALL = 32


def _expert_kernel(big, u_hbm, key_hbm, gsel_hbm, krow, cnt, w1_hbm, w3_hbm, w2_hbm, p_hbm, p_ref,
                   u_v, xs, zs, w1_v, w3_v, w2_v, mid, key_ref, gsel_ref, order, u_sem, k_sem, p_sem, w_sem):
    t, d = u_v.shape
    ng = t // GROUP
    u_copy = pltpu.make_async_copy(u_hbm, u_v, u_sem)
    u_copy.start()
    for e in range(EDEV):
        n = cnt[0, e] + cnt[1, e]
        rank = 0
        for f in range(EDEV):
            if f != e:
                m = cnt[0, f] + cnt[1, f]
                rank += ((m >= n) if f < e else (m > n)).astype(jnp.int32)
        order[rank] = e

    def copy(i, hbm, vm, k):
        s = lax.rem(i, 2)
        return pltpu.make_async_copy(hbm.at[order[i]], vm.at[s], w_sem.at[s, k])

    def w1_copy(i):
        return copy(i, w1_hbm, w1_v, 0)

    def w3_copy(i):
        return copy(i, w3_hbm, w3_v, 1)

    def w2_copy(i):
        return copy(i, w2_hbm, w2_v, 2)

    for i in range(2):
        w1_copy(i).start()
        w3_copy(i).start()
        w2_copy(i).start()
        if i == 0:
            k_copies = (pltpu.make_async_copy(key_hbm, key_ref, k_sem.at[0]),
                        pltpu.make_async_copy(gsel_hbm, gsel_ref, k_sem.at[1]))
            for cp in k_copies:
                cp.start()
    p_ref[...] = jnp.zeros_like(p_ref)
    u_copy.wait()
    lane = lax.broadcasted_iota(jnp.int32, (GROUP, 128), 1)

    def tokens(g):
        return pl.ds(g * GROUP if isinstance(g, int) else pl.multiple_of(g * GROUP, GROUP), GROUP)

    def pick(e, g, n):
        r = lax.broadcasted_iota(jnp.int32, (n, GROUP), 0).astype(F32)
        sel = jnp.where(krow[pl.ds(e, 1), tokens(g)] == r, 1.0, 0.0).astype(BF16)
        return jnp.dot(sel, u_v[tokens(g), :], preferred_element_type=F32).astype(BF16)

    def put(e, g, n, out):
        tl = tokens(g)
        r = lax.broadcasted_iota(jnp.int32, (GROUP, 128), 1).astype(F32)
        key = jnp.sum(jnp.where(lane == e, key_ref[tl, :], 0.0), axis=1, keepdims=True)
        sel = jnp.concatenate([jnp.where(key == r + 128.0 * q, 1.0, 0.0) for q in range(-(-n // 128))], axis=1)
        sel = sel[:, :n].astype(BF16)
        gt = jnp.sum(jnp.where(lane == e, gsel_ref[tl, :], 0.0), axis=1, keepdims=True)
        for q in range(d // 256):
            cs = slice(q * 256, (q + 1) * 256)
            back = jnp.dot(sel, out[:, cs], preferred_element_type=F32)
            p_ref[tl, cs] += back * gt

    def p_copy(g):
        return pltpu.make_async_copy(p_ref.at[tokens(g)], p_hbm.at[tokens(g)], p_sem.at[g])

    def done(i, g):
        @pl.when(i == EDEV - 1)
        def _():
            p_copy(g).start()

    def down(g, s):
        return jnp.dot(g, w2_v[s], preferred_element_type=F32).astype(BF16)

    @pl.loop(0, EDEV)
    def _(i):
        e, s = order[i], lax.rem(i, 2)
        most = jnp.maximum(cnt[0, e], cnt[1, e])
        few = jnp.logical_and(most > 0, most <= SMALL)
        many = most > SMALL
        both = slice(0, ng * SMALL)

        @pl.when(few)
        def _():
            for g in range(ng):
                xs[g * SMALL:(g + 1) * SMALL, :] = pick(e, g, SMALL)

        @pl.when(many)
        def _():
            for g in range(ng):
                xs[g * big:(g + 1) * big, :] = pick(e, g, big)

        w1_copy(i).wait()

        @pl.when(few)
        def _():
            zs[both, :] = jnp.dot(xs[both, :], w1_v[s], preferred_element_type=F32)

        @pl.when(many)
        def _():
            zs[...] = jnp.dot(xs[...], w1_v[s], preferred_element_type=F32)

        @pl.when(i + 2 < EDEV)
        def _():
            w1_copy(i + 2).start()

        w3_copy(i).wait()

        @pl.when(few)
        def _():
            mid[both, :] = _silu_mul(zs[both, :], jnp.dot(xs[both, :], w3_v[s], preferred_element_type=F32))

        @pl.when(many)
        def _():
            mid[...] = _silu_mul(zs[...], jnp.dot(xs[...], w3_v[s], preferred_element_type=F32))

        @pl.when(i + 2 < EDEV)
        def _():
            w3_copy(i + 2).start()

        w2_copy(i).wait()

        @pl.when(i == 0)
        def _():
            for cp in k_copies:
                cp.wait()

        @pl.when(few)
        def _():
            out = down(mid[both, :], s)
            for g in range(ng):
                put(e, g, SMALL, out[g * SMALL:(g + 1) * SMALL])
                done(i, g)

        @pl.when(many)
        def _():
            out = down(mid[...], s)
            for g in range(ng):
                put(e, g, big, out[g * big:(g + 1) * big])
                done(i, g)

        @pl.when(most == 0)
        def _():
            for g in range(ng):
                done(i, g)

        @pl.when(i + 2 < EDEV)
        def _():
            w2_copy(i + 2).start()

    for g in range(ng):
        p_copy(g).wait()


def _experts(u, key, gsel, krow, cnt, w1, w3, w2, blk):
    t, d = u.shape
    f = w1.shape[2]
    big = (blk - blk // 8) * (GROUP // blk)
    slots = big * (t // GROUP)
    return pl.pallas_call(
        functools.partial(_expert_kernel, big),
        out_shape=jax.ShapeDtypeStruct((t, d), F32),
        in_specs=[HBM, HBM, HBM, VMEM, SMEM, HBM, HBM, HBM],
        out_specs=HBM,
        scratch_shapes=[
            pltpu.VMEM((t, d), F32),
            pltpu.VMEM((t, d), BF16),
            pltpu.VMEM((slots, d), BF16),
            pltpu.VMEM((slots, f), F32),
            pltpu.VMEM((2, d, f), BF16),
            pltpu.VMEM((2, d, f), BF16),
            pltpu.VMEM((2, f, d), BF16),
            pltpu.VMEM((slots, f), BF16),
            pltpu.VMEM((t, 128), F32),
            pltpu.VMEM((t, 128), F32),
            pltpu.SMEM((EDEV,), jnp.int32),
            DMA(()), DMA((2,)), DMA((t // GROUP,)), DMA((2, 3)),
        ],
        compiler_params=pltpu.CompilerParams(vmem_limit_bytes=55 * 2 ** 20),
        name="experts",
    )(u, key, gsel, krow, cnt, w1, w3, w2)


COLS = ((0, 640), (640, 640), (1280, 768))
PARTS, ROWS = 4, 8
NS = 3 * PARTS


def _combine_kernel(p_hbm, g_ref, h_ref, u_ref, ws1_hbm, ws3_hbm, w_hbm, y_ref,
                    acc, r0, r1, r2, r3, w_v, a_v, b_v, late, sh, w_sem, a_sem, b_sem, p_sem,
                    s0, q0, s1, q1, s2, q2, s3, q3):
    z, y, x, c = _place()
    nw, _, wn = w_v.shape

    def w_copy(i):
        return pltpu.make_async_copy(w_hbm.at[:, pl.ds(i * wn, wn)], w_v.at[i], w_sem.at[i])

    streams = [(p, half) for half in range(PARTS) for p in range(3)]
    place = {0: x, 1: y, 2: z}

    def cols(p):
        return pl.ds(COLS[p][0], COLS[p][1])

    def rows(half):
        return pl.ds(half * ROWS, ROWS)

    early = g_ref.shape[1]

    def a_copy(i):
        return pltpu.make_async_copy(ws1_hbm.at[:, pl.ds(early + i * CH, CH)], a_v.at[i], a_sem.at[i])

    def b_copy(i):
        return pltpu.make_async_copy(ws3_hbm.at[:, pl.ds(early + i * CH, CH)], b_v.at[i], b_sem.at[i])

    def load(k):
        p, half = streams[k]
        return pltpu.make_async_copy(p_hbm.at[:, :, :, c, rows(half), cols(p)], acc.at[:, :, :, rows(half), cols(p)],
                                     p_sem.at[k])

    def swap(k):
        p, half = streams[k]
        return pltpu.make_async_remote_copy(
            p_hbm.at[:, :, :, 1 - c, rows(half), cols(p)], r0.at[:, :, :, rows(half), cols(p)], s0.at[k], q0.at[k],
            device_id=_dev(z, y, x, 1 - c), device_id_type=MESH)

    def region(ref, p, half, step, mine):
        ix = [pl.ds(0, 2)] * 3
        for s in range(step):
            dim = (p + s) % 3
            v = place[dim]
            ix[2 - dim] = v if (s < step - 1 or mine) else 1 - v
        return ref.at[ix[0], ix[1], ix[2], rows(half), cols(p)]

    def landing(p, half, step):
        ref = (r1, r2, r3)[step - 1]
        if step == 1:
            return ref.at[:, :, rows(half), cols(p)]
        if step == 2:
            return ref.at[:, rows(half), cols(p)]
        return ref.at[rows(half), cols(p)]

    def hop(k, step):
        p, half = streams[k]
        dim = (p + step - 1) % 3
        o = [z, y, x]
        o[2 - dim] = 1 - o[2 - dim]
        send, recv = ((s1, q1), (s2, q2), (s3, q3))[step - 1]
        return pltpu.make_async_remote_copy(
            region(acc, p, half, step, False), landing(p, half, step), send.at[k], recv.at[k],
            device_id=_dev(*o, c), device_id_type=MESH)

    for k in range(NS):
        load(k).start()
    for i in range(LATE):
        a_copy(i).start()
        b_copy(i).start()
    barrier = pltpu.get_barrier_semaphore()
    pl.semaphore_signal(barrier, inc=1, device_id=_dev(z, y, x, 1 - c), device_id_type=MESH)
    for d in (1, 2, 4):
        pl.semaphore_signal(barrier, inc=1, device_id=_dev(*_offset((z, y, x), d), c), device_id_type=MESH)
    pl.semaphore_wait(barrier, 4)
    for k in range(NS):
        swap(k).start()
    for i in range(nw):
        w_copy(i).start()

    def shared(i):
        w_copy(i).wait()
        cs = slice(i * wn, (i + 1) * wn)
        s = jnp.dot(g_ref[...], w_v[i, 0:early], preferred_element_type=F32)
        s += jnp.dot(late[...], w_v[i, early:], preferred_element_type=F32)
        sh[:, cs] = s + h_ref[:, cs].astype(F32)

    def up(i):
        a_copy(i).wait()
        b_copy(i).wait()
        late[:, i * CH:(i + 1) * CH] = _silu_mul(jnp.dot(u_ref[...], a_v[i], preferred_element_type=F32),
                                                 jnp.dot(u_ref[...], b_v[i], preferred_element_type=F32))

    for k in range(NS):
        p, half = streams[k]
        load(k).wait()
        swap(k).wait_recv()
        rs, cs = slice(half * ROWS, half * ROWS + ROWS), slice(COLS[p][0], COLS[p][0] + COLS[p][1])
        acc[:, :, :, rs, cs] += r0[:, :, :, rs, cs]
        hop(k, 1).start()
    for i in range(LATE):
        up(i)

    def add(k, step):
        p, half = streams[k]
        hop(k, step).wait_recv()
        v = region(acc, p, half, step, True)
        if step < 3:
            v[...] += landing(p, half, step)[...]
            hop(k, step + 1).start()
        else:
            tot = v[...] + landing(p, half, 3)[...]
            rs, cs = slice(half * ROWS, half * ROWS + ROWS), slice(COLS[p][0], COLS[p][0] + COLS[p][1])
            y_ref[rs, cs] = (sh[rs, cs] + tot).astype(BF16)

    for k in range(NS):
        add(k, 1)
        if k % 3 == 2:
            shared(k // 3)
        if k >= 6:
            add(k - 6, 2)
    for k in range(6, NS):
        add(k, 2)
    for k in range(NS):
        add(k, 3)
    for k in range(NS):
        swap(k).wait_send()
        for step in (1, 2, 3):
            hop(k, step).wait_send()


def _combine(part, g, h, u, ws1, ws3, ws2):
    b, d = h.shape
    fs = ws2.shape[0]
    nw = 4
    part = part.reshape(2, 2, 2, 2, b, d)
    return pl.pallas_call(
        _combine_kernel,
        out_shape=jax.ShapeDtypeStruct((b, d), BF16),
        in_specs=[HBM, VMEM, VMEM, VMEM, HBM, HBM, HBM],
        out_specs=VMEM,
        scratch_shapes=[
            pltpu.VMEM((2, 2, 2, b, d), F32),
            pltpu.VMEM((2, 2, 2, b, d), F32),
            pltpu.VMEM((2, 2, b, d), F32),
            pltpu.VMEM((2, b, d), F32),
            pltpu.VMEM((b, d), F32),
            pltpu.VMEM((nw, fs, d // nw), BF16),
            pltpu.VMEM((LATE, d, CH), BF16),
            pltpu.VMEM((LATE, d, CH), BF16),
            pltpu.VMEM((b, LATE * CH), BF16),
            pltpu.VMEM((b, d), F32),
            DMA((nw,)), DMA((LATE,)), DMA((LATE,)), DMA((NS,)),
            DMA((NS,)), DMA((NS,)), DMA((NS,)), DMA((NS,)), DMA((NS,)), DMA((NS,)), DMA((NS,)), DMA((NS,)),
        ],
        compiler_params=pltpu.CompilerParams(vmem_limit_bytes=50 * 2 ** 20, collective_id=1, has_side_effects=True),
        name="combine",
    )(part, g, h, u, ws1, ws3, ws2)


def solution(mesh):
    def body(x, kv_k, kv_v, lens, idx, gates, ln1, wq, wo, ln2, ws1, ws3, ws2, w1, w3, w2):
        b, d = x.shape
        h, u, uall, g, key, gsel, krow, cnt = _front(x, kv_k, kv_v, lens, idx, gates, ln1, ln2, wq, wo, ws1, ws3)
        part = _experts(uall.reshape(16 * b, d), key, gsel, krow, cnt, w1, w3, w2, b)
        return _combine(part, g, h, u, ws1, ws3, ws2)

    rows = P(GRP)
    rep = P()
    return jax.shard_map(
        body, mesh=mesh,
        in_specs=(rows, rows, rows, rows, rows, rows, rep, rep, rep, rep, rep, rep, rep, rows, rows, rows),
        out_specs=rows, check_vma=False)
```
